512 devices in a mesh: parts: 2 (over y), step: 32 (over z), frame: 4 (over x), head: 2 (over core).
Axes of the slice: x: 4, y: 2, z: 32, core: 2. Of those that a mesh axis runs over, the one named last changes fastest.
The devices are a block of a 4x8x32 slice.
Arguments:
- start_noise: float32 [32, 512], P('parts', 'frame'), parts along dimension 0, may hold values from -6 to 6
- position: bfloat16 [512, 1152], P('frame'), may hold values from -6 to 6
- time_table: bfloat16 [128, 1152], replicated, may hold values from -6 to 6
- time_index: int32 [32], P('step'), may hold values from 0 to 127
- sched_index: int32 [32], P('step'), may hold values from 0 to 127
- coef_keep: float32 [128], replicated, may hold values from -0.06 to -0.01
- coef_noise: float32 [128], replicated, may hold values from 0.03 to 0.12
- w_in: bfloat16 [16, 1152], replicated, may hold values from -1.5 to 1.5
- norm_gain: float32 [1152], replicated, may hold values from 0.5 to 1.5
- w_qkv: bfloat16 [1152, 3, 1152], P('step', None, 'head'), may hold values from -4 to 4
- w_proj: bfloat16 [1152, 1152], P('step', 'head'), may hold values from -0.1875 to 0.1875
- w_final: bfloat16 [16, 1152], replicated, may hold values from -0.1875 to 0.1875
Outputs:
- trajectory: float32 [32, 32, 512], P('step', 'parts', 'frame'), parts along dimension 1
- residual_norms: float32 [8], P('parts'), parts along dimension 0
The draws below stay inside these ranges and needn't reach their ends.
There are 2 independent parts, one for each index of `parts`. The reference program is written for one: setup_inputs(seed, part) draws one part's arguments, and reference() takes and returns one part's arrays. A program takes and returns all parts, laid end to end along the dimension named above; an argument that names none is the same for every part. Nothing has to cross between parts.
All inputs are finite; a program needn't handle non-finite values.
Results may differ from the reference program's by a relative error of at most 0.0044.
Values may be sent and summed in bfloat16 or wider, within the bound.
No kernel may reach another device: no remote copies, remote signals or barrier semaphores. Data moves between devices by JAX's collectives and lax.ppermute only.
A program may use at most 64 MiB of HBM per device.

```python
import math
import jax
import jax.numpy as jnp
from jax import lax

D = 1152
HEADS = 16
HDIM = 72
HQ = 1152
LAT_C = 16
NTOK = 512
STEPS = 32
SCHED = 128
ITERS = 4


def draw_w_qkv(key, part):
    base_key = jax.random.fold_in(jax.random.fold_in(key, 17), 0)
    base = jnp.clip(jax.random.normal(base_key, (D, 3, HQ), jnp.float32), -6.0, 6.0) * D ** (-0.5)
    return base.astype(jnp.bfloat16)


def place_ends(drawn, key, least, top_value):
    dims = drawn.shape
    place = [jax.random.randint(jax.random.fold_in(key, axis), (), 0, dims[axis]) for axis in range(len(dims))]
    drawn = drawn.at[tuple(place)].set(least)
    longest = dims.index(max(dims))
    place[longest] = (place[longest] + 1) % dims[longest]
    return drawn.at[tuple(place)].set(top_value)


def level_of(stream_key, shape, pieces, least, top_value):
    loudness, own = 1.0, jax.random.fold_in(stream_key, 6)
    for axis_at, parts in pieces:
        draws = jnp.exp(jax.random.uniform(jax.random.fold_in(own, axis_at), (parts,), jnp.float32, least / len(pieces), top_value / len(pieces)))
        loudness = loudness * jnp.repeat(draws, shape[axis_at] // parts).reshape([-1 if axis == axis_at else 1 for axis in range(len(shape))])
    return loudness


def scatter_about(own_key, dims, spread, most, shards=(), kind=jnp.bfloat16):
    array = spread * jax.random.normal(own_key, dims, jnp.float32)
    if shards:
        array = array * level_of(own_key, dims, shards, -0.22, 0.18)
    return jnp.clip(array, -most, most).astype(kind)


def setup_inputs(seed: int = 0, part: int = 0) -> dict:
    keys = jax.random.split(jax.random.key(seed), 13)
    part_keys = jax.random.split(jax.random.fold_in(keys[12], part), 13)
    start_noise = scatter_about(part_keys[0], (LAT_C, NTOK), 1.0, 6.0, ((1, 4),), jnp.float32)
    position = scatter_about(keys[1], (NTOK, D), 1.0, 6.0, ((0, 4),))
    time_table = scatter_about(keys[2], (SCHED, D), 1.0, 6.0)
    time_index = place_ends(jax.random.randint(keys[3], (STEPS,), 0, SCHED), jax.random.fold_in(keys[3], 1), 0, SCHED - 1).astype(jnp.int32)
    sched_index = place_ends(jax.random.randint(keys[4], (STEPS,), 0, SCHED), jax.random.fold_in(keys[4], 1), 0, SCHED - 1).astype(jnp.int32)
    coef_keep = jnp.clip(jax.random.uniform(keys[5], (SCHED,), jnp.float32, -0.06, -0.01), -0.06, -0.01)
    coef_noise = jnp.clip(jax.random.uniform(keys[6], (SCHED,), jnp.float32, 0.03, 0.12), 0.03, 0.12)
    w_in = scatter_about(keys[7], (LAT_C, D), LAT_C ** -0.5, 1.5)
    norm_gain = jnp.clip(1.0 + 0.1 * jax.random.normal(keys[8], (D,), jnp.float32), 0.5, 1.5)
    w_qkv = draw_w_qkv(jax.random.fold_in(keys[12], 71), part)
    w_proj = scatter_about(keys[10], (D, HQ), HQ ** -0.5, 0.1875, ((0, 32), (1, 2)))
    w_final = scatter_about(keys[11], (LAT_C, D), D ** -0.5, 0.1875)
    return dict(start_noise=start_noise, position=position, time_table=time_table, time_index=time_index, sched_index=sched_index, coef_keep=coef_keep, coef_noise=coef_noise, w_in=w_in, norm_gain=norm_gain, w_qkv=w_qkv, w_proj=w_proj, w_final=w_final)


def one_head(packed):
    queries, keys_part, values_part = packed
    scores = jnp.dot(queries, keys_part.T, preferred_element_type=jnp.float32) / math.sqrt(HDIM)
    top_score = lax.optimization_barrier(jnp.max(scores, axis=1, keepdims=True))
    weights_exp = jnp.exp(scores - top_score)
    totals = lax.optimization_barrier(jnp.sum(weights_exp, axis=1, keepdims=True))
    attended = jnp.dot(weights_exp.astype(jnp.bfloat16), values_part, preferred_element_type=jnp.float32)
    return (attended / totals).astype(jnp.bfloat16)

def denoise(latent, time_row, position, w_in, norm_gain, w_qkv, w_proj, w_final):
    latent_bf = latent.astype(jnp.bfloat16)
    hidden = jnp.dot(latent_bf.T, w_in, preferred_element_type=jnp.float32) + position.astype(jnp.float32) + time_row[None, :]
    normed = (hidden * lax.rsqrt(lax.optimization_barrier(jnp.mean(hidden * hidden, axis=1, keepdims=True)) + 1e-06) * norm_gain[None, :]).astype(jnp.bfloat16)
    projected = jnp.einsum('nd,dkq->nkq', normed.astype(jnp.float32), w_qkv.astype(jnp.float32)).astype(jnp.bfloat16)
    token_count = projected.shape[0]
    split_heads = projected.reshape(token_count, 3, HEADS, HDIM).transpose(1, 2, 0, 3)
    attended = lax.map(one_head, (split_heads[0], split_heads[1], split_heads[2]))
    attended = attended.transpose(1, 0, 2).reshape(token_count, HEADS * HDIM)
    branch = jnp.dot(attended, w_proj.T, preferred_element_type=jnp.float32)
    joined = (hidden + branch).astype(jnp.bfloat16)
    return jnp.dot(w_final, joined.T, preferred_element_type=jnp.float32)

def reference(start_noise, position, time_table, time_index, sched_index, coef_keep, coef_noise, w_in, norm_gain, w_qkv, w_proj, w_final):
    time_embed = time_table[time_index].astype(jnp.float32)
    keep_rate = coef_keep[sched_index]
    noise_rate = coef_noise[sched_index]
    states = jnp.broadcast_to(start_noise[None], (STEPS,) + start_noise.shape)

    def one_step(packed):
        return denoise(packed[0], packed[1], position, w_in, norm_gain, w_qkv, w_proj, w_final)
    residual_list = []
    drift_term = jnp.zeros_like(states)
    for iteration in range(ITERS):
        predicted = lax.map(one_step, (states, time_embed))
        drift_term = keep_rate[:, None, None] * states + noise_rate[:, None, None] * predicted
        running = jnp.cumsum(drift_term, axis=0)
        before = jnp.concatenate([jnp.zeros_like(running[:1]), running[:-1]], axis=0)
        new_states = start_noise[None] + before
        change = new_states - states
        residual_list.append(jnp.sqrt(jnp.mean(change * change) + 1e-06))
        states = new_states
    trajectory = states + drift_term
    return (trajectory, jnp.stack(residual_list))
```

```python
import functools
import math

import jax
import jax.numpy as jnp
from jax import lax
from jax.experimental import pallas as pl
from jax.experimental.pallas import tpu as pltpu
from jax.sharding import Mesh
from jax.sharding import PartitionSpec as P

HDIM = 72
ITERS = 4
ZLO = 4
F32 = jnp.float32
BF16 = jnp.bfloat16
STEP = ("zhi", "zlo")
HOOD = ("frame", "zlo", "head")


def three_parts(a):
    hi = lax.reduce_precision(a, 8, 7)
    mid = lax.reduce_precision(a - hi, 8, 7)
    return hi.astype(BF16), mid.astype(BF16), (a - hi - mid).astype(BF16)


def chosen(pieces, index):
    out = pieces[0]
    for at, piece in enumerate(pieces[1:], 1):
        out = jnp.where(index == at, piece, out)
    return out


def vmem_call(body, out_shape, *args, scratch=(), flops=0, name=None):
    spec = pl.BlockSpec(memory_space=pltpu.VMEM)
    return pl.pallas_call(
        body,
        out_shape=out_shape,
        in_specs=[spec] * len(args),
        out_specs=jax.tree.map(lambda _: spec, out_shape),
        scratch_shapes=list(scratch),
        cost_estimate=pl.CostEstimate(flops=flops, bytes_accessed=0, transcendentals=0),
        name=name,
    )(*args)


def eps_body(heads, steps, lat, x_ref, bext_ref, a_ref, c_ref, wfp_ref, out_ref, xs, es):
    cols = heads * HDIM
    tokens = x_ref.shape[0]
    width = bext_ref.shape[0] - lat - 3 * cols
    assert width == 0
    model = 1.0 / c_ref.shape[1]
    xs[...] = x_ref[...].astype(F32).T
    scale = math.log2(math.e) / math.sqrt(HDIM)
    ones16 = jnp.ones((lat, tokens), F32)
    ones8 = jnp.ones((8, tokens), F32)

    def one_step(step, carry):
        rows = pl.ds(pl.multiple_of(step * lat, lat), lat)
        x = xs[rows, :]
        xcat = jnp.concatenate([x, x, x, ones16], axis=0).astype(BF16)
        mixed = jnp.dot(a_ref[step], xcat, preferred_element_type=F32) + bext_ref[...]
        quad = mixed[3 * cols :, :]
        square = jnp.sum(x * quad, axis=0, keepdims=True) + c_ref[pl.ds(step, 1), :]
        rate = lax.rsqrt(jnp.maximum(square, 0.0) + 1e-06)
        outs = []
        for head in range(heads):
            q = mixed[head * HDIM : (head + 1) * HDIM, :]
            k = mixed[cols + head * HDIM : cols + (head + 1) * HDIM, :]
            v = mixed[2 * cols + head * HDIM : 2 * cols + (head + 1) * HDIM, :]
            q = (q * (rate * scale)).astype(BF16)
            k = (k * rate).astype(BF16)
            v = jnp.concatenate([v * rate, ones8], axis=0).astype(BF16)
            s = lax.dot_general(k, q, (((0,), (0,)), ((), ())), preferred_element_type=F32)
            top = jnp.max(s, axis=0, keepdims=True)
            e = jnp.exp2(s - top).astype(BF16)
            o = jnp.dot(v, e, preferred_element_type=F32)
            outs.append(o[:HDIM, :] * (1.0 / o[HDIM : HDIM + 1, :]))
        o = jnp.concatenate(outs, axis=0).astype(BF16)
        part = jnp.dot(wfp_ref[...], o, preferred_element_type=F32)
        es[rows, :] = part[:lat, :] + part[lat:, :]
        return carry

    lax.fori_loop(0, steps, one_step, 0)
    out_ref[...] = es[...].T.astype(BF16)


def eps_part(x, bext, a_all, c_all, wfp, lat):
    steps = a_all.shape[0]
    tokens = x.shape[0]
    heads = wfp.shape[1] // HDIM
    flops = 2 * steps * tokens * (bext.shape[0] * 64 + heads * tokens * 160)
    return vmem_call(
        functools.partial(eps_body, heads, steps, lat),
        jax.ShapeDtypeStruct((tokens, steps * lat), BF16),
        x,
        bext,
        a_all,
        c_all,
        wfp,
        scratch=(
            pltpu.VMEM((steps * lat, tokens), F32),
            pltpu.VMEM((steps * lat, tokens), F32),
        ),
        flops=flops,
        name="eps_part",
    )


def advance(lat, frames, cores, got_ref, x_ref, noise_ref, base_ref, fblk_ref, coef_ref):
    groups, rows, lanes = x_ref.shape
    lane = lax.broadcasted_iota(jnp.int32, (rows, lanes), 1)
    before = jnp.zeros((rows, lanes), F32)
    drifts, states = [], []
    square = jnp.zeros((rows, lanes), F32)
    for group in range(groups):
        old = x_ref[group]
        total = base_ref[group]
        for frame in range(frames):
            for core in range(cores):
                member = (frame * groups + group) * cores + core
                total = total + got_ref[member].astype(F32)
        xb = old.astype(BF16)
        total = total + jnp.dot(
            jnp.concatenate([xb, xb, xb], axis=1), fblk_ref[...], preferred_element_type=F32
        )
        drift = (
            coef_ref[pl.ds(group, 1), :] * old + coef_ref[pl.ds(groups + group, 1), :] * total
        )
        running = drift
        shift = lat
        while shift < lanes:
            running = running + jnp.where(lane >= shift, pltpu.roll(running, shift, 1), 0.0)
            shift *= 2
        own = jnp.where(lane >= lat, pltpu.roll(running, lat, 1), 0.0)
        new = noise_ref[...] + before + own
        last = jnp.where(lane >= lanes - lat, running, 0.0)
        shift = lanes // 2
        while shift >= lat:
            last = last + pltpu.roll(last, shift, 1)
            shift //= 2
        before = before + last
        change = new - old
        square = square + change * change
        drifts.append(drift)
        states.append(new)
    return drifts, states, square


def glue_body(lat, frames, cores, got_ref, x_ref, noise_ref, base_ref, fblk_ref, coef_ref,
              new_ref, send_ref, square_ref):
    _, states, square = advance(
        lat, frames, cores, got_ref, x_ref, noise_ref, base_ref, fblk_ref, coef_ref
    )
    square_ref[...] = square
    groups = len(states)
    for group, new in enumerate(states):
        new_ref[group] = new
        rounded = new.astype(BF16)
        for frame in range(frames):
            for core in range(cores):
                send_ref[(frame * groups + group) * cores + core] = rounded


def last_body(lat, frames, cores, where_ref, got_ref, x_ref, noise_ref, base_ref, fblk_ref,
              coef_ref, sq0_ref, sq1_ref, sq2_ref, send_ref):
    drifts, states, square = advance(
        lat, frames, cores, got_ref, x_ref, noise_ref, base_ref, fblk_ref, coef_ref
    )
    groups, rows, lanes = x_ref.shape
    half = rows // 2
    zhi = where_ref[0]
    width = groups * lat
    first = zhi * groups
    per_group = lanes // lat
    picked = chosen([s + d for s, d in zip(states, drifts)], first // per_group)
    offset = lax.rem(first, per_group) * lat
    lane = lax.broadcasted_iota(jnp.int32, (half, lanes), 1)
    turn = lax.rem(lanes - offset, lanes)
    top = pltpu.roll(picked[:half], turn, 1)
    bottom = pltpu.roll(picked[half:], lax.rem(turn + width, lanes), 1)
    piece = jnp.where(lane < width, top, bottom)
    sums = jnp.zeros((half, lanes), F32)
    inner = lax.rem(lane, lat)
    for at, sq in enumerate((sq0_ref[...], sq1_ref[...], sq2_ref[...], square)):
        sums = jnp.where(inner == at, jnp.sum(sq), sums)
    for group in range(groups):
        slot = (group + 1) % groups
        mixed = jnp.where(lane // lat == slot, sums, piece)
        for frame in range(frames):
            for core in range(cores):
                send_ref[(frame * groups + group) * cores + core] = mixed


def end_body(lat, frames, cores, cells, where_ref, got_ref, traj_ref, norm_ref):
    members, half, lanes = got_ref.shape
    groups = members // (frames * cores)
    frame, zlo = where_ref[1], where_ref[2]
    width = groups * lat
    everyone = got_ref[0]
    for member in range(1, members):
        everyone = everyone + got_ref[member]
    slot = lax.rem(zlo + 1, groups)
    sums = pltpu.roll(everyone, lax.rem(lanes - slot * lat, lanes), 1)
    norm_ref[...] = jnp.sqrt(sums / cells + 1e-06)
    rows = []
    back = lax.rem(lanes - zlo * lat, lanes)
    for own in range(groups * cores):
        piece = got_ref[frame * (groups * cores) + own]
        rows.append(pltpu.roll(piece, back, 1))
        rows.append(pltpu.roll(piece, lax.rem(back + lanes - width, lanes), 1))
    traj_ref[...] = jnp.concatenate(rows, axis=0).T[:lat, :]


def smem_first(body, out_shape, where, *args, name=None):
    spec = pl.BlockSpec(memory_space=pltpu.VMEM)
    return pl.pallas_call(
        body,
        out_shape=out_shape,
        in_specs=[pl.BlockSpec(memory_space=pltpu.SMEM)] + [spec] * len(args),
        out_specs=jax.tree.map(lambda _: spec, out_shape),
        name=name,
    )(where, *args)


def local(
    start_noise,
    position,
    time_table,
    time_index,
    sched_index,
    coef_keep,
    coef_noise,
    w_in,
    norm_gain,
    w_qkv,
    w_proj,
    w_final,
):
    lat, row_count = start_noise.shape
    rows_d = w_qkv.shape[0]
    model = position.shape[1]
    frames, cores = lax.axis_size("frame"), lax.axis_size("head")
    zlo_n, zhi_n = lax.axis_size("zlo"), lax.axis_size("zhi")
    step_n = zlo_n * zhi_n
    steps = step_n // zlo_n
    tokens = row_count * frames
    cols = w_qkv.shape[2] // frames
    heads = cols // HDIM
    members = frames * zlo_n * cores
    mine = tokens // members
    lanes = steps * lat
    frame, zlo, zhi, core = (lax.axis_index(a) for a in ("frame", "zlo", "zhi", "head"))
    step = zhi * zlo_n + zlo

    proj_mine = chosen([w_proj[:, f * cols : (f + 1) * cols] for f in range(frames)], frame)
    final_mine = lax.dynamic_slice_in_dim(w_final, step * rows_d, rows_d, 1)
    mix = jnp.dot(final_mine, proj_mine, preferred_element_type=F32)
    mix = lax.all_to_all(mix.reshape(zlo_n, lat // zlo_n, cols), "zlo", 0, 0, tiled=True)
    mix = jnp.sum(mix, axis=0).T.astype(BF16)

    qkv_mine = chosen([w_qkv[:, :, f * cols : (f + 1) * cols] for f in range(frames)], frame)
    main = [qkv_mine[:, k, :lanes] for k in range(3)]
    rest = jnp.concatenate([qkv_mine[:, k, lanes:] for k in range(3)], axis=1)
    tall = rows_d // 2
    pieces = cols // tall
    side = jnp.concatenate(
        [rest[:tall], rest[tall:]] + [mix[g * tall : (g + 1) * tall] for g in range(pieces)], axis=1
    )
    index_row = jnp.concatenate([time_index, sched_index]).astype(BF16)
    index_row = jnp.pad(index_row, (0, lanes - 2))[None]
    payload = jnp.concatenate(main + [side, index_row], axis=0)
    gathered = lax.all_gather(payload, STEP, axis=0)

    noise_rows = jnp.pad(start_noise.astype(BF16), ((0, 0), (0, model - row_count)))
    frame_load = jnp.concatenate([position, noise_rows], axis=0)
    frame_all = lax.all_to_all(
        jnp.broadcast_to(frame_load[None], (frames, *frame_load.shape)), "frame", 0, 0, tiled=True
    )
    positions = frame_all[:, :row_count].reshape(tokens, model)
    noise_all = frame_all[:, row_count:, :row_count]

    w_main = [
        gathered[:, k * rows_d : (k + 1) * rows_d].reshape(step_n * rows_d, lanes) for k in range(3)
    ]
    sides = gathered[:, 3 * rows_d : 3 * rows_d + tall]
    extra = cols - lanes
    w_rest = jnp.concatenate([sides[:, :, : 3 * extra], sides[:, :, 3 * extra : 6 * extra]], axis=1)
    w_rest = w_rest.reshape(step_n * rows_d, 3 * extra)
    part = lat // zlo_n
    mixes = sides[:, :, 6 * extra :].astype(F32).reshape(zhi_n, zlo_n, tall, pieces, part)
    mixes = jnp.sum(mixes, axis=0).transpose(0, 3, 2, 1).reshape(lat, cols)
    mix_hi = lax.reduce_precision(mixes, 8, 7)
    wfp = jnp.concatenate([mix_hi, mixes - mix_hi], axis=0).astype(BF16)
    table_rows = time_table.shape[0]
    indices = gathered[:, 3 * rows_d + tall, :2].astype(F32)
    spots = jnp.arange(table_rows, dtype=F32)
    pick_time = (indices[:, :1] == spots[None]).astype(BF16)
    pick_sched = (indices[:, 1:] == spots[None]).astype(F32)
    temb_all = jnp.dot(pick_time, time_table, preferred_element_type=F32).astype(BF16)
    keep = jnp.sum(pick_sched * coef_keep[None], axis=1)
    rate = jnp.sum(pick_sched * coef_noise[None], axis=1)
    coef = jnp.repeat(jnp.concatenate([keep, rate]).reshape(2 * zlo_n, steps), lat, axis=1)
    temb = lax.dynamic_slice_in_dim(temb_all, zlo * steps, steps, 0)

    every = jnp.concatenate([positions, w_in, temb], axis=0)
    scaled = every.astype(F32) * norm_gain[None]
    scaled_hi = lax.reduce_precision(scaled, 8, 7)
    scaled_lo = (scaled - scaled_hi).astype(BF16)
    scaled_hi = scaled_hi.astype(BF16)

    def against(w):
        dims = (((0,), (1,)), ((), ()))
        return lax.dot_general(w, scaled_hi, dims, preferred_element_type=F32) + lax.dot_general(
            w, scaled_lo, dims, preferred_element_type=F32
        )

    thin = against(w_rest)
    blocks = []
    for k in range(3):
        blocks += [against(w_main[k]), thin[k * extra : (k + 1) * extra]]
    gram = lax.dot_general(
        jnp.concatenate([w_in, temb], axis=0),
        every,
        (((1,), (1,)), ((), ())),
        preferred_element_type=F32,
    )
    inv = 1.0 / model
    linear = jnp.concatenate(
        blocks + [gram[:lat] * jnp.where(jnp.arange(every.shape[0]) // lat == tokens // lat, inv, 2 * inv)],
        axis=0,
    )
    bext = linear[:, :tokens]
    latent = linear[:, tokens : tokens + lat]
    time_part = linear[:, tokens + lat :]
    latent_parts = jnp.concatenate(three_parts(latent), axis=1)
    time_parts = jnp.stack(three_parts(time_part.T), axis=2)
    a_all = jnp.concatenate(
        [
            jnp.broadcast_to(latent_parts[None], (steps, *latent_parts.shape)),
            jnp.pad(time_parts, ((0, 0), (0, 0), (0, lat - 3))),
        ],
        axis=2,
    )
    wide = positions.astype(F32)
    temb_wide = temb.astype(F32)
    c_all = (
        jnp.sum(wide * wide, axis=1)[None]
        + 2.0 * gram[lat:, :tokens]
        + jnp.sum(temb_wide * temb_wide, axis=1)[:, None]
    ) * inv

    at = (zlo * cores + core) * mine
    own_position = lax.dynamic_slice_in_dim(position, at, mine, 0)
    own_noise = lax.dynamic_slice_in_dim(start_noise, at, mine, 1).T
    nt = (((1,), (1,)), ((), ()))
    base_own = lax.dot_general(own_position, w_final, nt, preferred_element_type=F32)
    base_time = lax.dot_general(temb_all, w_final, nt, preferred_element_type=F32)
    base = jnp.tile(base_own, (1, steps))[None] + base_time.reshape(zlo_n, 1, lanes)
    final_in = lax.dot_general(w_in, w_final, nt, preferred_element_type=F32)
    fblk = jnp.concatenate(
        [jnp.kron(jnp.eye(steps, dtype=F32), p.astype(F32)) for p in three_parts(final_in)], axis=0
    ).astype(BF16)
    noise = jnp.tile(own_noise, (1, steps))
    states = jnp.broadcast_to(noise[None], (zlo_n, mine, lanes))
    x = jnp.tile(noise_all.transpose(0, 2, 1).reshape(tokens, lat), (1, steps))

    squares = []
    where = jnp.stack([zhi, frame, zlo]).astype(jnp.int32)
    for iteration in range(ITERS):
        part_eps = eps_part(x, bext, a_all, c_all, wfp, lat)
        got = lax.all_to_all(part_eps.reshape(members, mine, lanes), HOOD, 0, 0, tiled=True)
        if iteration < ITERS - 1:
            states, send, square = vmem_call(
                functools.partial(glue_body, lat, frames, cores),
                (
                    jax.ShapeDtypeStruct(states.shape, F32),
                    jax.ShapeDtypeStruct((members, mine, lanes), BF16),
                    jax.ShapeDtypeStruct((mine, lanes), F32),
                ),
                got,
                states,
                noise,
                base,
                fblk,
                coef,
                name="advance",
            )
            squares.append(square)
            x = lax.all_to_all(send, HOOD, 0, 0, tiled=True).reshape(tokens, lanes)
        else:
            send = smem_first(
                functools.partial(last_body, lat, frames, cores),
                jax.ShapeDtypeStruct((members, mine // 2, lanes), F32),
                where,
                got,
                states,
                noise,
                base,
                fblk,
                coef,
                *squares,
                name="last",
            )
    ended = lax.all_to_all(send, HOOD, 0, 0, tiled=True)
    trajectory, norms = smem_first(
        functools.partial(end_body, lat, frames, cores, float(step_n * lat * tokens)),
        (
            jax.ShapeDtypeStruct((lat, row_count), F32),
            jax.ShapeDtypeStruct((mine // 2, lanes), F32),
        ),
        where,
        ended,
        name="end",
    )
    return trajectory[None], norms[0, :ITERS]


def solution(mesh):
    names = ("parts", "zhi", "zlo", "frame", "head")
    sizes = mesh.shape
    devices = mesh.devices.reshape(
        sizes["parts"], sizes["step"] // ZLO, ZLO, sizes["frame"], sizes["head"]
    )
    return jax.shard_map(
        local,
        mesh=Mesh(devices, names),
        in_specs=(
            P("parts", "frame"),
            P("frame", None),
            P(),
            P(STEP),
            P(STEP),
            P(),
            P(),
            P(),
            P(),
            P(STEP, None, "head"),
            P(STEP, "head"),
            P(),
        ),
        out_specs=(P(STEP, "parts", "frame"), P("parts")),
        check_vma=False,
    )
```

```python
import functools
import math

import jax
import jax.numpy as jnp
from jax import lax
from jax.experimental import pallas as pl
from jax.experimental.pallas import tpu as pltpu
from jax.sharding import Mesh
from jax.sharding import PartitionSpec as P

HDIM = 72
ITERS = 4
ZLO = 4
GRANT = 16 * 1024 * 1024
F32 = jnp.float32
BF16 = jnp.bfloat16
STEP = ("zhi", "zlo")
HOOD = ("frame", "zlo", "head")


def chosen(pieces, index):
    out = pieces[0]
    for at, piece in enumerate(pieces[1:], 1):
        out = jnp.where(index == at, piece, out)
    return out


def vmem_call(body, out_shape, *args, scratch=(), flops=0, name=None):
    spec = pl.BlockSpec(memory_space=pltpu.VMEM)
    return pl.pallas_call(
        body,
        out_shape=out_shape,
        in_specs=[spec] * len(args),
        out_specs=jax.tree.map(lambda _: spec, out_shape),
        scratch_shapes=list(scratch),
        cost_estimate=pl.CostEstimate(flops=flops, bytes_accessed=0, transcendentals=0),
        compiler_params=pltpu.CompilerParams(vmem_limit_bytes=GRANT),
        name=name,
    )(*args)


def eps_body(heads, steps, lat, x_ref, bext_ref, a_ref, c_ref, wfp_ref, out_ref, xs, es, qs, ks, vs, os, s0, s1, m0, m1):
    cols = heads * HDIM
    tokens = x_ref.shape[0]
    xs[...] = x_ref[...].astype(F32).T
    scale = math.log2(math.e) / math.sqrt(HDIM)
    eight = lax.broadcasted_iota(jnp.int32, (steps, tokens), 0)
    blank = jnp.zeros((a_ref.shape[1] - 3 * (lat + steps), tokens), F32)
    ones8 = jnp.ones((8, tokens), F32)
    held, tops = (s0, s1), (m0, m1)

    def project(step, carry):
        rows = pl.ds(pl.multiple_of(step * lat, lat), lat)
        x = xs[rows, :]
        pick = jnp.where(eight == step, 1.0, 0.0)
        xcat = jnp.concatenate([x, x, x, pick, pick, pick, blank], axis=0).astype(BF16)
        mixed = jnp.dot(a_ref[...], xcat, preferred_element_type=F32) + bext_ref[...]
        quad = mixed[3 * cols :, :]
        square = jnp.sum(x * quad, axis=0, keepdims=True) + c_ref[pl.ds(step, 1), :]
        rate = lax.rsqrt(jnp.maximum(square, 0.0) + 1e-06)
        for head in range(heads):
            q, k, v = (
                mixed[part * cols + head * HDIM : part * cols + (head + 1) * HDIM, :]
                for part in range(3)
            )
            qs[step, head] = (q * (rate * scale)).astype(BF16)
            ks[step, head] = (k * rate).astype(BF16)
            vs[step, head] = jnp.concatenate([v * rate, ones8], axis=0).astype(BF16)
        return carry

    lax.fori_loop(0, steps, project, 0, unroll=True)

    def score(step, head):
        s = lax.dot_general(
            ks[step, head], qs[step, head], (((0,), (0,)), ((), ())), preferred_element_type=F32
        )
        held[head % 2][...] = s
        tops[head % 2][...] = jnp.max(s, axis=0, keepdims=True)

    def weigh(step, head):
        e = jnp.exp2(held[head % 2][...] - tops[head % 2][...]).astype(BF16)
        os[step, head] = jnp.dot(vs[step, head], e, preferred_element_type=F32)

    score(0, 0)

    def attend(step, carry):
        for head in range(heads):
            if head + 1 < heads:
                score(step, head + 1)
            else:
                score(jnp.minimum(step + 1, steps - 1), 0)
            weigh(step, head)
        return carry

    lax.fori_loop(0, steps, attend, 0, unroll=2)

    for step in range(steps):
        outs = []
        for head in range(heads):
            o = os[step, head]
            outs.append(o[:HDIM, :] * (1.0 / o[HDIM : HDIM + 1, :]))
        o = jnp.concatenate(outs, axis=0).astype(BF16)
        part = jnp.dot(wfp_ref[...], o, preferred_element_type=F32)
        es[step * lat : (step + 1) * lat, :] = part[:lat, :] + part[lat:, :]
    out_ref[...] = es[...].T.astype(BF16)


def eps_part(x, bext, a_all, c_all, wfp, lat):
    steps = c_all.shape[0]
    tokens = x.shape[0]
    heads = wfp.shape[1] // HDIM
    flops = 2 * steps * tokens * (bext.shape[0] * 64 + heads * tokens * 160)
    return vmem_call(
        functools.partial(eps_body, heads, steps, lat),
        jax.ShapeDtypeStruct((tokens, steps * lat), BF16),
        x,
        bext,
        a_all,
        c_all,
        wfp,
        scratch=(
            pltpu.VMEM((steps * lat, tokens), F32),
            pltpu.VMEM((steps * lat, tokens), F32),
            pltpu.VMEM((steps, heads, HDIM, tokens), BF16),
            pltpu.VMEM((steps, heads, HDIM, tokens), BF16),
            pltpu.VMEM((steps, heads, HDIM + 8, tokens), BF16),
            pltpu.VMEM((steps, heads, HDIM + 8, tokens), F32),
            pltpu.VMEM((tokens, tokens), F32),
            pltpu.VMEM((tokens, tokens), F32),
            pltpu.VMEM((1, tokens), F32),
            pltpu.VMEM((1, tokens), F32),
        ),
        flops=flops,
        name="eps_part",
    )


def advance(lat, frames, cores, got_ref, x_ref, noise_ref, base_ref, fblk_ref, coef_ref):
    groups, rows, lanes = x_ref.shape
    lane = lax.broadcasted_iota(jnp.int32, (rows, lanes), 1)
    before = jnp.zeros((rows, lanes), F32)
    drifts, states = [], []
    square = jnp.zeros((rows, lanes), F32)
    for group in range(groups):
        old = x_ref[group]
        total = base_ref[group]
        for frame in range(frames):
            for core in range(cores):
                member = (frame * groups + group) * cores + core
                total = total + got_ref[member].astype(F32)
        xb = old.astype(BF16)
        total = total + jnp.dot(
            jnp.concatenate([xb, xb, xb], axis=1), fblk_ref[...], preferred_element_type=F32
        )
        drift = (
            coef_ref[pl.ds(group, 1), :] * old + coef_ref[pl.ds(groups + group, 1), :] * total
        )
        running = drift
        shift = lat
        while shift < lanes:
            running = running + jnp.where(lane >= shift, pltpu.roll(running, shift, 1), 0.0)
            shift *= 2
        own = jnp.where(lane >= lat, pltpu.roll(running, lat, 1), 0.0)
        new = noise_ref[...] + before + own
        last = jnp.where(lane >= lanes - lat, running, 0.0)
        shift = lanes // 2
        while shift >= lat:
            last = last + pltpu.roll(last, shift, 1)
            shift //= 2
        before = before + last
        change = new - old
        square = square + change * change
        drifts.append(drift)
        states.append(new)
    return drifts, states, square


def glue_body(lat, frames, cores, got_ref, x_ref, noise_ref, base_ref, fblk_ref, coef_ref,
              new_ref, send_ref, square_ref):
    _, states, square = advance(
        lat, frames, cores, got_ref, x_ref, noise_ref, base_ref, fblk_ref, coef_ref
    )
    square_ref[...] = square
    groups = len(states)
    for group, new in enumerate(states):
        new_ref[group] = new
        rounded = new.astype(BF16)
        for frame in range(frames):
            for core in range(cores):
                send_ref[(frame * groups + group) * cores + core] = rounded


def last_body(lat, frames, cores, where_ref, got_ref, x_ref, noise_ref, base_ref, fblk_ref,
              coef_ref, sq0_ref, sq1_ref, sq2_ref, send_ref):
    drifts, states, square = advance(
        lat, frames, cores, got_ref, x_ref, noise_ref, base_ref, fblk_ref, coef_ref
    )
    groups, rows, lanes = x_ref.shape
    half = rows // 2
    zhi = where_ref[0]
    width = groups * lat
    first = zhi * groups
    per_group = lanes // lat
    picked = chosen([s + d for s, d in zip(states, drifts)], first // per_group)
    offset = lax.rem(first, per_group) * lat
    lane = lax.broadcasted_iota(jnp.int32, (half, lanes), 1)
    turn = lax.rem(lanes - offset, lanes)
    top = pltpu.roll(picked[:half], turn, 1)
    bottom = pltpu.roll(picked[half:], lax.rem(turn + width, lanes), 1)
    piece = jnp.where(lane < width, top, bottom)
    sums = jnp.zeros((half, lanes), F32)
    inner = lax.rem(lane, lat)
    for at, sq in enumerate((sq0_ref[...], sq1_ref[...], sq2_ref[...], square)):
        sums = jnp.where(inner == at, jnp.sum(sq), sums)
    for group in range(groups):
        slot = (group + 1) % groups
        mixed = jnp.where(lane // lat == slot, sums, piece)
        for frame in range(frames):
            for core in range(cores):
                send_ref[(frame * groups + group) * cores + core] = mixed


def end_body(lat, frames, cores, cells, where_ref, got_ref, traj_ref, norm_ref):
    members, half, lanes = got_ref.shape
    groups = members // (frames * cores)
    frame, zlo = where_ref[1], where_ref[2]
    width = groups * lat
    everyone = got_ref[0]
    for member in range(1, members):
        everyone = everyone + got_ref[member]
    slot = lax.rem(zlo + 1, groups)
    sums = pltpu.roll(everyone, lax.rem(lanes - slot * lat, lanes), 1)
    norm_ref[...] = jnp.sqrt(sums / cells + 1e-06)
    rows = []
    back = lax.rem(lanes - zlo * lat, lanes)
    for own in range(groups * cores):
        piece = got_ref[frame * (groups * cores) + own]
        rows.append(pltpu.roll(piece, back, 1))
        rows.append(pltpu.roll(piece, lax.rem(back + lanes - width, lanes), 1))
    traj_ref[...] = jnp.concatenate(rows, axis=0).T[:lat, :]


def smem_first(body, out_shape, where, *args, scratch=(), name=None):
    spec = pl.BlockSpec(memory_space=pltpu.VMEM)
    return pl.pallas_call(
        body,
        out_shape=out_shape,
        in_specs=[pl.BlockSpec(memory_space=pltpu.SMEM)] + [spec] * len(args),
        out_specs=jax.tree.map(lambda _: spec, out_shape),
        scratch_shapes=list(scratch),
        compiler_params=pltpu.CompilerParams(vmem_limit_bytes=GRANT),
        name=name,
    )(where, *args)


def split_two(a):
    hi = a.astype(BF16)
    return hi, (a - hi.astype(F32)).astype(BF16)


def split_lanes(a, lat, steps):
    hi = a.astype(BF16).astype(F32)
    mid = (a - hi).astype(BF16).astype(F32)
    low = a - hi - mid
    lane = lax.broadcasted_iota(jnp.int32, a.shape, 1)
    first, second, third = 3 * lat, 3 * lat + steps, 3 * lat + 2 * steps
    is_hi = (lane < lat) | ((lane >= first) & (lane < second))
    is_mid = ((lane >= lat) & (lane < 2 * lat)) | ((lane >= second) & (lane < third))
    return jnp.where(is_hi, hi, jnp.where(is_mid, mid, low)).astype(BF16)


def prep_body(lat, cores, extra, where_ref, w_ref, all_ref, position_ref, start_ref, index_ref,
              table_ref, gain_ref, keep_ref, rate_ref, w_in_ref, final_ref,
              bext_ref, a_ref, c_ref, base_ref, fblk_ref, coef_ref, noise_ref, state_ref, x_ref,
              temb_ref, turned_ref):
    zlo, core = where_ref[2], where_ref[3]
    frames = all_ref.shape[0]
    rows, model = position_ref.shape
    groups, mine, lanes = base_ref.shape
    steps = lanes // lat
    count = groups * steps
    inv = 1.0 / model
    nt = (((1,), (1,)), ((), ()))

    def nt_dot(a, b):
        return lax.dot_general(a, b, nt, preferred_element_type=F32)

    spots = lax.broadcasted_iota(jnp.int32, (count, table_ref.shape[0]), 1).astype(F32)
    pick_time = jnp.where(index_ref[:, 0:1] == spots, 1.0, 0.0).astype(BF16)
    pick_sched = jnp.where(index_ref[:, 1:2] == spots, 1.0, 0.0)
    temb_all = jnp.dot(pick_time, table_ref[...], preferred_element_type=F32)
    temb_ref[...] = temb_all
    temb = temb_ref[pl.ds(pl.multiple_of(zlo * steps, steps), steps), :]
    lane = lax.broadcasted_iota(jnp.int32, (count, lanes), 1)
    own = lax.broadcasted_iota(jnp.int32, (count, lanes), 0)
    here = (lane // lat) == lax.rem(own, steps)

    def spread(a):
        return jnp.sum(jnp.where(here, a, 0.0).reshape(groups, steps, lanes), axis=1)

    keep = jnp.sum(pick_sched * keep_ref[...], axis=1, keepdims=True)
    rate = jnp.sum(pick_sched * rate_ref[...], axis=1, keepdims=True)
    coef_ref[:groups] = spread(jnp.broadcast_to(keep, (count, lanes)))
    coef_ref[groups:] = spread(jnp.broadcast_to(rate, (count, lanes)))

    final = final_ref[...].astype(F32)
    final = jnp.concatenate([final] * steps, axis=0).astype(BF16)
    w_in = w_in_ref[...].astype(F32)
    w_in_all = jnp.concatenate([w_in] * steps, axis=0).astype(BF16)
    mixed = nt_dot(w_in_all, final)
    square_lane = lax.broadcasted_iota(jnp.int32, (lanes, lanes), 1) // lat
    square_row = lax.broadcasted_iota(jnp.int32, (lanes, lanes), 0) // lat
    mixed = jnp.where(square_lane == square_row, mixed, 0.0)
    hi = mixed.astype(BF16)
    mid = (mixed - hi.astype(F32)).astype(BF16)
    fblk_ref[:lanes] = hi
    fblk_ref[lanes : 2 * lanes] = mid
    fblk_ref[2 * lanes :] = (mixed - hi.astype(F32) - mid.astype(F32)).astype(BF16)
    at = pl.multiple_of((zlo * cores + core) * mine, mine)
    base_own = nt_dot(position_ref[pl.ds(at, mine), :], final)
    base_time = spread(nt_dot(temb_all.astype(BF16), final))
    for group in range(groups):
        base_ref[group] = base_own + base_time[group : group + 1, :]

    turned_ref[...] = jnp.concatenate([start_ref[...]] * steps, axis=0).T
    noise = turned_ref[pl.ds(at, mine), :]
    noise_ref[...] = noise
    for group in range(groups):
        state_ref[group] = noise
    for frame in range(frames):
        noise = all_ref[frame, rows:, :rows].astype(F32)
        x_ref[frame * rows : (frame + 1) * rows] = (
            jnp.concatenate([noise] * steps, axis=0).T.astype(BF16)
        )

    blank = jnp.zeros((lanes - 3 * (lat + steps), model), F32)
    thin = jnp.concatenate([w_in, w_in, w_in, temb, temb, temb, blank], axis=0)
    thin_bf = thin.astype(BF16)
    gain = gain_ref[...]
    w = w_ref[...]
    thin_hi, thin_lo = split_two(thin * gain)
    linear = jnp.dot(thin_hi, w, preferred_element_type=F32) + jnp.dot(
        thin_lo, w, preferred_element_type=F32
    )
    places = []
    for part in range(3):
        places += [(part * lanes, lanes), (3 * lanes + part * extra, extra)]
    row = 0
    turned = linear.T
    for start, size in places:
        a_ref[row : row + size] = split_lanes(turned[start : start + size], lat, steps)
        row += size
    gram = nt_dot(thin_bf[:lat], thin_bf)
    gram_lane = lax.broadcasted_iota(jnp.int32, gram.shape, 1)
    gram = gram * jnp.where(gram_lane < 3 * lat, inv, 2.0 * inv)
    a_ref[row:] = split_lanes(gram, lat, steps)
    temb_square = jnp.sum(temb * temb, axis=1, keepdims=True)
    for frame in range(frames):
        there = pl.ds(frame * rows, rows)
        tokens_bf = all_ref[frame, :rows, :]
        wide = tokens_bf.astype(F32)
        wide_hi, wide_lo = split_two(wide * gain)
        linear = (
            jnp.dot(wide_hi, w, preferred_element_type=F32)
            + jnp.dot(wide_lo, w, preferred_element_type=F32)
        ).T
        row = 0
        for start, size in places:
            bext_ref[row : row + size, frame * rows : (frame + 1) * rows] = linear[
                start : start + size
            ]
            row += size
        gram = nt_dot(thin_bf, tokens_bf)
        bext_ref[row:, frame * rows : (frame + 1) * rows] = gram[:lat] * (2.0 * inv)
        square = wide * wide
        folded = square[:, :lanes]
        for chunk in range(1, model // lanes):
            folded = folded + square[:, chunk * lanes : (chunk + 1) * lanes]
        square = jnp.sum(folded.T, axis=0, keepdims=True)
        c_ref[:, frame * rows : (frame + 1) * rows] = inv * (
            square + 2.0 * gram[3 * lat : 3 * lat + steps] + temb_square
        )


def local(
    start_noise,
    position,
    time_table,
    time_index,
    sched_index,
    coef_keep,
    coef_noise,
    w_in,
    norm_gain,
    w_qkv,
    w_proj,
    w_final,
):
    lat, row_count = start_noise.shape
    rows_d = w_qkv.shape[0]
    model = position.shape[1]
    frames, cores = lax.axis_size("frame"), lax.axis_size("head")
    zlo_n, zhi_n = lax.axis_size("zlo"), lax.axis_size("zhi")
    step_n = zlo_n * zhi_n
    steps = step_n // zlo_n
    tokens = row_count * frames
    cols = w_qkv.shape[2] // frames
    heads = cols // HDIM
    members = frames * zlo_n * cores
    mine = tokens // members
    lanes = steps * lat
    frame, zlo, zhi, core = (lax.axis_index(a) for a in ("frame", "zlo", "zhi", "head"))
    step = zhi * zlo_n + zlo

    proj_mine = chosen([w_proj[:, f * cols : (f + 1) * cols] for f in range(frames)], frame)
    final_mine = lax.dynamic_slice_in_dim(w_final, step * rows_d, rows_d, 1)
    mix = jnp.dot(final_mine, proj_mine, preferred_element_type=F32)
    mix = lax.all_to_all(mix.reshape(zlo_n, lat // zlo_n, cols), "zlo", 0, 0, tiled=True)
    mix = jnp.sum(mix, axis=0).T.astype(BF16)

    qkv_mine = chosen([w_qkv[:, :, f * cols : (f + 1) * cols] for f in range(frames)], frame)
    main = [qkv_mine[:, k, :lanes] for k in range(3)]
    rest = jnp.concatenate([qkv_mine[:, k, lanes:] for k in range(3)], axis=1)
    tall = rows_d // 2
    pieces = cols // tall
    side = jnp.concatenate(
        [rest[:tall], rest[tall:]] + [mix[g * tall : (g + 1) * tall] for g in range(pieces)], axis=1
    )
    index_row = jnp.concatenate([time_index, sched_index]).astype(BF16)
    index_row = jnp.pad(index_row, (0, lanes - 2))[None]
    payload = jnp.concatenate(main + [side, index_row], axis=0)
    gathered = lax.all_gather(payload, STEP, axis=0)

    noise_rows = jnp.pad(start_noise.astype(BF16), ((0, 0), (0, model - row_count)))
    frame_load = jnp.concatenate([position, noise_rows], axis=0)
    frame_all = lax.all_to_all(
        jnp.broadcast_to(frame_load[None], (frames, *frame_load.shape)), "frame", 0, 0, tiled=True
    )
    sides = gathered[:, 3 * rows_d : 3 * rows_d + tall]
    extra = cols - lanes
    w_rest = jnp.concatenate([sides[:, :, : 3 * extra], sides[:, :, 3 * extra : 6 * extra]], axis=1)
    w_rest = jnp.pad(w_rest, ((0, 0), (0, 0), (0, lanes - 3 * extra)))
    w_all = jnp.concatenate(
        [gathered[:, k * rows_d : (k + 1) * rows_d] for k in range(3)] + [w_rest], axis=2
    ).reshape(step_n * rows_d, 4 * lanes)
    part = lat // zlo_n
    mixes = sides[:, :, 6 * extra :].astype(F32).reshape(zhi_n, zlo_n, tall, pieces, part)
    mixes = jnp.sum(mixes, axis=0).transpose(0, 3, 2, 1).reshape(lat, cols)
    mix_hi = lax.reduce_precision(mixes, 8, 7)
    wfp = jnp.concatenate([mix_hi, mixes - mix_hi], axis=0).astype(BF16)
    index_rows = gathered[:, 3 * rows_d + tall].astype(F32)

    where = jnp.stack([zhi, frame, zlo, core]).astype(jnp.int32)
    bext, a_all, c_all, base, fblk, coef, noise, states, x = smem_first(
        functools.partial(prep_body, lat, cores, extra),
        (
            jax.ShapeDtypeStruct((3 * cols + lat, tokens), F32),
            jax.ShapeDtypeStruct((3 * cols + lat, lanes), BF16),
            jax.ShapeDtypeStruct((steps, tokens), F32),
            jax.ShapeDtypeStruct((zlo_n, mine, lanes), F32),
            jax.ShapeDtypeStruct((3 * lanes, lanes), BF16),
            jax.ShapeDtypeStruct((2 * zlo_n, lanes), F32),
            jax.ShapeDtypeStruct((mine, lanes), F32),
            jax.ShapeDtypeStruct((zlo_n, mine, lanes), F32),
            jax.ShapeDtypeStruct((tokens, lanes), BF16),
        ),
        where,
        w_all,
        frame_all,
        position,
        start_noise,
        index_rows,
        time_table,
        norm_gain[None],
        coef_keep[None],
        coef_noise[None],
        w_in,
        w_final,
        scratch=(pltpu.VMEM((step_n, model), F32), pltpu.VMEM((row_count, lanes), F32)),
        name="prep",
    )

    squares = []
    for iteration in range(ITERS):
        part_eps = eps_part(x, bext, a_all, c_all, wfp, lat)
        got = lax.all_to_all(part_eps.reshape(members, mine, lanes), HOOD, 0, 0, tiled=True)
        if iteration < ITERS - 1:
            states, send, square = vmem_call(
                functools.partial(glue_body, lat, frames, cores),
                (
                    jax.ShapeDtypeStruct(states.shape, F32),
                    jax.ShapeDtypeStruct((members, mine, lanes), BF16),
                    jax.ShapeDtypeStruct((mine, lanes), F32),
                ),
                got,
                states,
                noise,
                base,
                fblk,
                coef,
                name="advance",
            )
            squares.append(square)
            x = lax.all_to_all(send, HOOD, 0, 0, tiled=True).reshape(tokens, lanes)
        else:
            send = smem_first(
                functools.partial(last_body, lat, frames, cores),
                jax.ShapeDtypeStruct((members, mine // 2, lanes), F32),
                where,
                got,
                states,
                noise,
                base,
                fblk,
                coef,
                *squares,
                name="last",
            )
    ended = lax.all_to_all(send, HOOD, 0, 0, tiled=True)
    trajectory, norms = smem_first(
        functools.partial(end_body, lat, frames, cores, float(step_n * lat * tokens)),
        (
            jax.ShapeDtypeStruct((lat, row_count), F32),
            jax.ShapeDtypeStruct((mine // 2, lanes), F32),
        ),
        where,
        ended,
        name="end",
    )
    return trajectory[None], norms[0, :ITERS]


def solution(mesh):
    names = ("parts", "zhi", "zlo", "frame", "head")
    sizes = mesh.shape
    devices = mesh.devices.reshape(
        sizes["parts"], sizes["step"] // ZLO, ZLO, sizes["frame"], sizes["head"]
    )
    return jax.shard_map(
        local,
        mesh=Mesh(devices, names),
        in_specs=(
            P("parts", "frame"),
            P("frame", None),
            P(),
            P(STEP),
            P(STEP),
            P(),
            P(),
            P(),
            P(),
            P(STEP, None, "head"),
            P(STEP, "head"),
            P(),
        ),
        out_specs=(P(STEP, "parts", "frame"), P("parts")),
        check_vma=False,
    )
```

```python
import functools
import math

import jax
import jax.numpy as jnp
from jax import lax
from jax.experimental import pallas as pl
from jax.experimental.pallas import tpu as pltpu
from jax.sharding import Mesh
from jax.sharding import PartitionSpec as P

HDIM = 72
ITERS = 4
ZLO = 4
GRANT = 16 * 1024 * 1024
F32 = jnp.float32
BF16 = jnp.bfloat16
STEP = ("zhi", "zlo")
HOOD = ("frame", "zlo", "head")


def chosen(pieces, index):
    out = pieces[0]
    for at, piece in enumerate(pieces[1:], 1):
        out = jnp.where(index == at, piece, out)
    return out


def vmem_call(body, out_shape, *args, scratch=(), flops=0, name=None):
    spec = pl.BlockSpec(memory_space=pltpu.VMEM)
    return pl.pallas_call(
        body,
        out_shape=out_shape,
        in_specs=[spec] * len(args),
        out_specs=jax.tree.map(lambda _: spec, out_shape),
        scratch_shapes=list(scratch),
        cost_estimate=pl.CostEstimate(flops=flops, bytes_accessed=0, transcendentals=0),
        compiler_params=pltpu.CompilerParams(vmem_limit_bytes=GRANT),
        name=name,
    )(*args)


def eps_body(heads, steps, lat, x_ref, bext_ref, a_ref, c_ref, wfp_ref, out_ref, xs, es, qs, ks, vs, os, s0, s1, m0, m1):
    cols = heads * HDIM
    tokens = x_ref.shape[0]
    xs[...] = x_ref[...].astype(F32).T
    scale = math.log2(math.e) / math.sqrt(HDIM)
    eight = lax.broadcasted_iota(jnp.int32, (steps, tokens), 0)
    blank = jnp.zeros((a_ref.shape[1] - 3 * (lat + steps), tokens), F32)
    ones8 = jnp.ones((8, tokens), F32)
    held, tops = (s0, s1), (m0, m1)

    lanes_pad = 128

    def project(step, carry):
        rows = pl.ds(pl.multiple_of(step * lat, lat), lat)
        x = xs[rows, :]
        pick = jnp.where(eight == step, 1.0, 0.0)
        xcat = jnp.concatenate([x, x, x, pick, pick, pick, blank], axis=0).astype(BF16)
        mixed = jnp.dot(a_ref[...], xcat, preferred_element_type=F32) + bext_ref[...]
        quad = mixed[3 * cols :, :]
        square = jnp.sum(x * quad, axis=0, keepdims=True) + c_ref[pl.ds(step, 1), :]
        rate = lax.rsqrt(jnp.maximum(square, 0.0) + 1e-06)
        for head in range(heads):
            q, k, v = (
                mixed[part * cols + head * HDIM : part * cols + (head + 1) * HDIM, :]
                for part in range(3)
            )
            qs[step, head] = (q * (rate * scale)).astype(BF16)
            ks[step, head] = (jnp.concatenate([k * rate, jnp.zeros((lanes_pad - HDIM, tokens), F32)], axis=0).T).astype(BF16)
            vs[step, head] = jnp.concatenate([v * rate, ones8], axis=0).astype(BF16)
        return carry

    lax.fori_loop(0, steps, project, 0, unroll=True)

    def score(step, head):
        s = jnp.dot(ks[step, head][:, :HDIM], qs[step, head], preferred_element_type=F32)
        held[head % 2][...] = s
        tops[head % 2][...] = jnp.max(s, axis=0, keepdims=True)

    def weigh(step, head):
        e = jnp.exp2(held[head % 2][...] - tops[head % 2][...]).astype(BF16)
        os[step, head] = jnp.dot(vs[step, head], e, preferred_element_type=F32)

    score(0, 0)

    def attend(step, carry):
        for head in range(heads):
            if head + 1 < heads:
                score(step, head + 1)
            else:
                score(jnp.minimum(step + 1, steps - 1), 0)
            weigh(step, head)
        return carry

    lax.fori_loop(0, steps, attend, 0, unroll=2)

    for step in range(steps):
        outs = []
        for head in range(heads):
            o = os[step, head]
            outs.append(o[:HDIM, :] * (1.0 / o[HDIM : HDIM + 1, :]))
        o = jnp.concatenate(outs, axis=0).astype(BF16)
        part = jnp.dot(wfp_ref[...], o, preferred_element_type=F32)
        es[step * lat : (step + 1) * lat, :] = part[:lat, :] + part[lat:, :]
    out_ref[...] = es[...].T.astype(BF16)


def eps_part(x, bext, a_all, c_all, wfp, lat):
    steps = c_all.shape[0]
    tokens = x.shape[0]
    heads = wfp.shape[1] // HDIM
    flops = 2 * steps * tokens * (bext.shape[0] * 64 + heads * tokens * 160)
    return vmem_call(
        functools.partial(eps_body, heads, steps, lat),
        jax.ShapeDtypeStruct((tokens, steps * lat), BF16),
        x,
        bext,
        a_all,
        c_all,
        wfp,
        scratch=(
            pltpu.VMEM((steps * lat, tokens), F32),
            pltpu.VMEM((steps * lat, tokens), F32),
            pltpu.VMEM((steps, heads, HDIM, tokens), BF16),
            pltpu.VMEM((steps, heads, tokens, 128), BF16),
            pltpu.VMEM((steps, heads, HDIM + 8, tokens), BF16),
            pltpu.VMEM((steps, heads, HDIM + 8, tokens), F32),
            pltpu.VMEM((tokens, tokens), F32),
            pltpu.VMEM((tokens, tokens), F32),
            pltpu.VMEM((1, tokens), F32),
            pltpu.VMEM((1, tokens), F32),
        ),
        flops=flops,
        name="eps_part",
    )


def advance(lat, frames, cores, got_ref, x_ref, noise_ref, base_ref, fblk_ref, coef_ref):
    groups, rows, lanes = x_ref.shape
    lane = lax.broadcasted_iota(jnp.int32, (rows, lanes), 1)
    before = jnp.zeros((rows, lanes), F32)
    drifts, states = [], []
    square = jnp.zeros((rows, lanes), F32)
    for group in range(groups):
        old = x_ref[group]
        total = base_ref[group]
        for frame in range(frames):
            for core in range(cores):
                member = (frame * groups + group) * cores + core
                total = total + got_ref[member].astype(F32)
        xb = old.astype(BF16)
        total = total + jnp.dot(
            jnp.concatenate([xb, xb, xb], axis=1), fblk_ref[...], preferred_element_type=F32
        )
        drift = (
            coef_ref[pl.ds(group, 1), :] * old + coef_ref[pl.ds(groups + group, 1), :] * total
        )
        running = drift
        shift = lat
        while shift < lanes:
            running = running + jnp.where(lane >= shift, pltpu.roll(running, shift, 1), 0.0)
            shift *= 2
        own = jnp.where(lane >= lat, pltpu.roll(running, lat, 1), 0.0)
        new = noise_ref[...] + before + own
        last = jnp.where(lane >= lanes - lat, running, 0.0)
        shift = lanes // 2
        while shift >= lat:
            last = last + pltpu.roll(last, shift, 1)
            shift //= 2
        before = before + last
        change = new - old
        square = square + change * change
        drifts.append(drift)
        states.append(new)
    return drifts, states, square


def glue_body(lat, frames, cores, got_ref, x_ref, noise_ref, base_ref, fblk_ref, coef_ref,
              new_ref, send_ref, square_ref):
    _, states, square = advance(
        lat, frames, cores, got_ref, x_ref, noise_ref, base_ref, fblk_ref, coef_ref
    )
    square_ref[...] = square
    groups = len(states)
    for group, new in enumerate(states):
        new_ref[group] = new
        rounded = new.astype(BF16)
        for frame in range(frames):
            for core in range(cores):
                send_ref[(frame * groups + group) * cores + core] = rounded


def last_body(lat, frames, cores, where_ref, got_ref, x_ref, noise_ref, base_ref, fblk_ref,
              coef_ref, sq0_ref, sq1_ref, sq2_ref, send_ref):
    drifts, states, square = advance(
        lat, frames, cores, got_ref, x_ref, noise_ref, base_ref, fblk_ref, coef_ref
    )
    groups, rows, lanes = x_ref.shape
    half = rows // 2
    zhi = where_ref[0]
    width = groups * lat
    first = zhi * groups
    per_group = lanes // lat
    picked = chosen([s + d for s, d in zip(states, drifts)], first // per_group)
    offset = lax.rem(first, per_group) * lat
    lane = lax.broadcasted_iota(jnp.int32, (half, lanes), 1)
    turn = lax.rem(lanes - offset, lanes)
    top = pltpu.roll(picked[:half], turn, 1)
    bottom = pltpu.roll(picked[half:], lax.rem(turn + width, lanes), 1)
    piece = jnp.where(lane < width, top, bottom)
    sums = jnp.zeros((half, lanes), F32)
    inner = lax.rem(lane, lat)
    for at, sq in enumerate((sq0_ref[...], sq1_ref[...], sq2_ref[...], square)):
        sums = jnp.where(inner == at, jnp.sum(sq), sums)
    for group in range(groups):
        slot = (group + 1) % groups
        mixed = jnp.where(lane // lat == slot, sums, piece)
        for frame in range(frames):
            for core in range(cores):
                send_ref[(frame * groups + group) * cores + core] = mixed


def end_body(lat, frames, cores, cells, where_ref, got_ref, traj_ref, norm_ref):
    members, half, lanes = got_ref.shape
    groups = members // (frames * cores)
    frame, zlo = where_ref[1], where_ref[2]
    width = groups * lat
    everyone = got_ref[0]
    for member in range(1, members):
        everyone = everyone + got_ref[member]
    slot = lax.rem(zlo + 1, groups)
    sums = pltpu.roll(everyone, lax.rem(lanes - slot * lat, lanes), 1)
    norm_ref[...] = jnp.sqrt(sums / cells + 1e-06)
    rows = []
    back = lax.rem(lanes - zlo * lat, lanes)
    for own in range(groups * cores):
        piece = got_ref[frame * (groups * cores) + own]
        rows.append(pltpu.roll(piece, back, 1))
        rows.append(pltpu.roll(piece, lax.rem(back + lanes - width, lanes), 1))
    traj_ref[...] = jnp.concatenate(rows, axis=0).T[:lat, :]


def smem_first(body, out_shape, where, *args, scratch=(), name=None):
    spec = pl.BlockSpec(memory_space=pltpu.VMEM)
    return pl.pallas_call(
        body,
        out_shape=out_shape,
        in_specs=[pl.BlockSpec(memory_space=pltpu.SMEM)] + [spec] * len(args),
        out_specs=jax.tree.map(lambda _: spec, out_shape),
        scratch_shapes=list(scratch),
        compiler_params=pltpu.CompilerParams(vmem_limit_bytes=GRANT),
        name=name,
    )(where, *args)


def split_two(a):
    hi = a.astype(BF16)
    return hi, (a - hi.astype(F32)).astype(BF16)


def split_lanes(a, lat, steps):
    hi = a.astype(BF16).astype(F32)
    mid = (a - hi).astype(BF16).astype(F32)
    low = a - hi - mid
    lane = lax.broadcasted_iota(jnp.int32, a.shape, 1)
    first, second, third = 3 * lat, 3 * lat + steps, 3 * lat + 2 * steps
    is_hi = (lane < lat) | ((lane >= first) & (lane < second))
    is_mid = ((lane >= lat) & (lane < 2 * lat)) | ((lane >= second) & (lane < third))
    return jnp.where(is_hi, hi, jnp.where(is_mid, mid, low)).astype(BF16)


def prep_body(lat, cores, extra, where_ref, got_ref, all_ref, position_ref, start_ref, table_ref,
              gain_ref, keep_ref, rate_ref, w_in_ref, final_ref, bext_ref, a_ref, c_ref, base_ref, fblk_ref, coef_ref, noise_ref, state_ref, x_ref,
              temb_ref, turned_ref, w_ref, index_ref):
    zlo, core = where_ref[2], where_ref[3]
    frames = all_ref.shape[0]
    rows, model = position_ref.shape
    groups, mine, lanes = base_ref.shape
    steps = lanes // lat
    count = groups * steps
    inv = 1.0 / model
    nt = (((1,), (1,)), ((), ()))

    def nt_dot(a, b):
        return lax.dot_general(a, b, nt, preferred_element_type=F32)

    rows_d = model // count
    tall = rows_d // 2
    for source in range(count):
        got = got_ref[source].astype(F32)
        at = source * rows_d
        for part in range(3):
            w_ref[at : at + rows_d, part * lanes : (part + 1) * lanes] = got[
                part * rows_d : (part + 1) * rows_d
            ]
        side = got[3 * rows_d : 3 * rows_d + tall]
        w_ref[at : at + tall, 3 * lanes :] = side
        w_ref[at + tall : at + rows_d, 3 * lanes :] = jnp.concatenate(
            [side[:, 3 * extra :], side[:, : 3 * extra]], axis=1
        )
        index_ref[source : source + 1] = got[3 * rows_d + tall : 3 * rows_d + tall + 1]

    spots = lax.broadcasted_iota(jnp.int32, (count, table_ref.shape[0]), 1).astype(F32)
    pick_time = jnp.where(index_ref[:, 0:1] == spots, 1.0, 0.0).astype(BF16)
    pick_sched = jnp.where(index_ref[:, 1:2] == spots, 1.0, 0.0)
    temb_all = jnp.dot(pick_time, table_ref[...], preferred_element_type=F32)
    temb_ref[...] = temb_all
    temb = temb_ref[pl.ds(pl.multiple_of(zlo * steps, steps), steps), :]
    lane = lax.broadcasted_iota(jnp.int32, (count, lanes), 1)
    own = lax.broadcasted_iota(jnp.int32, (count, lanes), 0)
    here = (lane // lat) == lax.rem(own, steps)

    def spread(a):
        return jnp.sum(jnp.where(here, a, 0.0).reshape(groups, steps, lanes), axis=1)

    keep = jnp.sum(pick_sched * keep_ref[...], axis=1, keepdims=True)
    rate = jnp.sum(pick_sched * rate_ref[...], axis=1, keepdims=True)
    coef_ref[:groups] = spread(jnp.broadcast_to(keep, (count, lanes)))
    coef_ref[groups:] = spread(jnp.broadcast_to(rate, (count, lanes)))

    final = final_ref[...].astype(F32)
    final = jnp.concatenate([final] * steps, axis=0).astype(BF16)
    w_in = w_in_ref[...].astype(F32)
    w_in_all = jnp.concatenate([w_in] * steps, axis=0).astype(BF16)
    mixed = nt_dot(w_in_all, final)
    square_lane = lax.broadcasted_iota(jnp.int32, (lanes, lanes), 1) // lat
    square_row = lax.broadcasted_iota(jnp.int32, (lanes, lanes), 0) // lat
    mixed = jnp.where(square_lane == square_row, mixed, 0.0)
    hi = mixed.astype(BF16)
    mid = (mixed - hi.astype(F32)).astype(BF16)
    fblk_ref[:lanes] = hi
    fblk_ref[lanes : 2 * lanes] = mid
    fblk_ref[2 * lanes :] = (mixed - hi.astype(F32) - mid.astype(F32)).astype(BF16)
    at = pl.multiple_of((zlo * cores + core) * mine, mine)
    base_own = nt_dot(position_ref[pl.ds(at, mine), :], final)
    base_time = spread(nt_dot(temb_all.astype(BF16), final))
    for group in range(groups):
        base_ref[group] = base_own + base_time[group : group + 1, :]

    turned_ref[...] = jnp.concatenate([start_ref[...]] * steps, axis=0).T
    noise = turned_ref[pl.ds(at, mine), :]
    noise_ref[...] = noise
    for group in range(groups):
        state_ref[group] = noise
    for frame in range(frames):
        noise = all_ref[frame, rows:, :rows].astype(F32)
        x_ref[frame * rows : (frame + 1) * rows] = (
            jnp.concatenate([noise] * steps, axis=0).T.astype(BF16)
        )

    blank = jnp.zeros((lanes - 3 * (lat + steps), model), F32)
    thin = jnp.concatenate([w_in, w_in, w_in, temb, temb, temb, blank], axis=0)
    thin_bf = thin.astype(BF16)
    gain = gain_ref[...]
    w = w_ref[...].astype(BF16)
    thin_hi, thin_lo = split_two(thin * gain)
    linear = jnp.dot(thin_hi, w, preferred_element_type=F32) + jnp.dot(
        thin_lo, w, preferred_element_type=F32
    )
    places = []
    for part in range(3):
        places += [(part * lanes, lanes), (3 * lanes + part * extra, extra)]
    row = 0
    turned = linear.T
    for start, size in places:
        a_ref[row : row + size] = split_lanes(turned[start : start + size], lat, steps)
        row += size
    gram = nt_dot(thin_bf[:lat], thin_bf)
    gram_lane = lax.broadcasted_iota(jnp.int32, gram.shape, 1)
    gram = gram * jnp.where(gram_lane < 3 * lat, inv, 2.0 * inv)
    a_ref[row:] = split_lanes(gram, lat, steps)
    temb_square = jnp.sum(temb * temb, axis=1, keepdims=True)
    for frame in range(frames):
        there = pl.ds(frame * rows, rows)
        tokens_bf = all_ref[frame, :rows, :]
        wide = tokens_bf.astype(F32)
        wide_hi, wide_lo = split_two(wide * gain)
        linear = (
            jnp.dot(wide_hi, w, preferred_element_type=F32)
            + jnp.dot(wide_lo, w, preferred_element_type=F32)
        ).T
        row = 0
        for start, size in places:
            bext_ref[row : row + size, frame * rows : (frame + 1) * rows] = linear[
                start : start + size
            ]
            row += size
        gram = nt_dot(thin_bf, tokens_bf)
        bext_ref[row:, frame * rows : (frame + 1) * rows] = gram[:lat] * (2.0 * inv)
        square = wide * wide
        folded = square[:, :lanes]
        for chunk in range(1, model // lanes):
            folded = folded + square[:, chunk * lanes : (chunk + 1) * lanes]
        square = jnp.sum(folded.T, axis=0, keepdims=True)
        c_ref[:, frame * rows : (frame + 1) * rows] = inv * (
            square + 2.0 * gram[3 * lat : 3 * lat + steps] + temb_square
        )


def exact_pick(values, wanted):
    return jnp.dot(values, jnp.where(wanted, 1.0, 0.0).astype(BF16), preferred_element_type=F32)


def pack_body(extra, where_ref, qkv_ref, proj_ref, final_ref, start_ref, position_ref,
              mix_ref, frame_ref, main_ref, rows_ref, half_ref):
    frame, step = where_ref[1], where_ref[4]
    lat, rows = start_ref.shape
    rows_d, width = proj_ref.shape
    frames, parts = frame_ref.shape[0], mix_ref.shape[0]
    lanes = main_ref.shape[1]
    cols = mix_ref.shape[2]
    tall = rows_d // 2

    column = lax.broadcasted_iota(jnp.int32, (width, 2 * lanes), 0) - frame * cols
    lane = lax.broadcasted_iota(jnp.int32, (width, 2 * lanes), 1)
    both = column == lane
    model = final_ref.shape[1]
    feature = lax.broadcasted_iota(jnp.int32, (model, lanes), 0) - step * rows_d
    final = exact_pick(final_ref[...], feature == lax.broadcasted_iota(jnp.int32, (model, lanes), 1))
    proj = exact_pick(proj_ref[...], both)
    blank = jnp.zeros((lanes - rows_d, 2 * lanes), F32)
    proj = jnp.concatenate([proj, blank], axis=0).astype(BF16)
    feature_lane = lax.broadcasted_iota(jnp.int32, final.shape, 1)
    final = jnp.where(feature_lane < rows_d, final, 0.0).astype(BF16)
    mix = jnp.dot(final, proj, preferred_element_type=F32)
    each = lat // parts
    for part in range(parts):
        mix_ref[part] = mix[part * each : (part + 1) * each, :cols]

    noise = jnp.concatenate(
        [start_ref[...], jnp.zeros((lat, model - rows), F32)], axis=1
    ).astype(BF16)
    for at in range(frames):
        frame_ref[at, :rows] = position_ref[...]
        frame_ref[at, rows:] = noise

    side = jnp.zeros((rows_d, 2 * lanes), F32)
    for part in range(3):
        weights = qkv_ref[part]
        rows_ref[part * rows_d : (part + 1) * rows_d, :] = exact_pick(weights, both)[:, :lanes]
        shifted = lane - part * extra
        first = (column - lanes == shifted) & (shifted >= 0) & (shifted < extra)
        shifted = lane - lanes - (3 + part) * extra
        second = (column - lanes == shifted) & (shifted >= 0) & (shifted < extra)
        side = side + exact_pick(weights, first | second)
    half_ref[...] = side[:, lanes:]
    rows_ref[3 * rows_d : 3 * rows_d + tall, :] = side[:tall, :lanes] + half_ref[tall:, :]
    spot = lax.broadcasted_iota(jnp.int32, (1, lanes), 1)
    times = where_ref[5].astype(F32)
    plans = where_ref[6].astype(F32)
    rows_ref[3 * rows_d + tall : 3 * rows_d + tall + 1, :] = jnp.where(
        spot == 0, times, jnp.where(spot == 1, plans, 0.0)
    )
    main_ref[...] = rows_ref[...][: main_ref.shape[0], :].astype(BF16)


def local(
    start_noise,
    position,
    time_table,
    time_index,
    sched_index,
    coef_keep,
    coef_noise,
    w_in,
    norm_gain,
    w_qkv,
    w_proj,
    w_final,
):
    lat, row_count = start_noise.shape
    rows_d = w_qkv.shape[0]
    model = position.shape[1]
    frames, cores = lax.axis_size("frame"), lax.axis_size("head")
    zlo_n, zhi_n = lax.axis_size("zlo"), lax.axis_size("zhi")
    step_n = zlo_n * zhi_n
    steps = step_n // zlo_n
    tokens = row_count * frames
    cols = w_qkv.shape[2] // frames
    heads = cols // HDIM
    members = frames * zlo_n * cores
    mine = tokens // members
    lanes = steps * lat
    frame, zlo, zhi, core = (lax.axis_index(a) for a in ("frame", "zlo", "zhi", "head"))
    step = zhi * zlo_n + zlo

    where = jnp.concatenate(
        [jnp.stack([zhi, frame, zlo, core, step]).astype(jnp.int32), time_index, sched_index]
    )
    tall = rows_d // 2
    extra = cols - lanes
    pieces = cols // tall
    payload_rows = 3 * rows_d + tall + 1
    mix, frame_load, payload = smem_first(
        functools.partial(pack_body, extra),
        (
            jax.ShapeDtypeStruct((zlo_n, lat // zlo_n, cols), F32),
            jax.ShapeDtypeStruct((frames, row_count + lat, model), BF16),
            jax.ShapeDtypeStruct((payload_rows, lanes), BF16),
        ),
        where,
        w_qkv.transpose(1, 0, 2),
        w_proj,
        w_final,
        start_noise,
        position,
        scratch=(pltpu.VMEM((payload_rows + 1, lanes), F32), pltpu.VMEM((rows_d, lanes), F32)),
        name="pack",
    )

    mix = jnp.sum(lax.all_to_all(mix, "zlo", 0, 0, tiled=True), axis=0)
    mix = mix.reshape(lat // zlo_n, pieces, tall).transpose(2, 1, 0).reshape(tall, -1)
    payload = payload + jnp.pad(
        mix.astype(BF16), ((3 * rows_d, 1), (6 * extra, lanes - 6 * extra - mix.shape[1]))
    )

    frame_all = lax.all_to_all(frame_load, "frame", 0, 0, tiled=True)

    gathered = lax.all_gather(payload, STEP, axis=0)

    sides = gathered[:, 3 * rows_d : 3 * rows_d + tall]
    part = lat // zlo_n
    mixes = sides[:, :, 6 * extra :].astype(F32).reshape(zhi_n, zlo_n, tall, pieces, part)
    mixes = jnp.sum(mixes, axis=0).transpose(0, 3, 2, 1).reshape(lat, cols)
    mix_hi = lax.reduce_precision(mixes, 8, 7)
    wfp = jnp.concatenate([mix_hi, mixes - mix_hi], axis=0).astype(BF16)
    bext, a_all, c_all, base, fblk, coef, noise, states, x = smem_first(
        functools.partial(prep_body, lat, cores, extra),
        (
            jax.ShapeDtypeStruct((3 * cols + lat, tokens), F32),
            jax.ShapeDtypeStruct((3 * cols + lat, lanes), BF16),
            jax.ShapeDtypeStruct((steps, tokens), F32),
            jax.ShapeDtypeStruct((zlo_n, mine, lanes), F32),
            jax.ShapeDtypeStruct((3 * lanes, lanes), BF16),
            jax.ShapeDtypeStruct((2 * zlo_n, lanes), F32),
            jax.ShapeDtypeStruct((mine, lanes), F32),
            jax.ShapeDtypeStruct((zlo_n, mine, lanes), F32),
            jax.ShapeDtypeStruct((tokens, lanes), BF16),
        ),
        where,
        gathered,
        frame_all,
        position,
        start_noise,
        time_table,
        norm_gain[None],
        coef_keep[None],
        coef_noise[None],
        w_in,
        w_final,
        scratch=(
            pltpu.VMEM((step_n, model), F32),
            pltpu.VMEM((row_count, lanes), F32),
            pltpu.VMEM((step_n * rows_d, 4 * lanes), F32),
            pltpu.VMEM((step_n, lanes), F32),
        ),
        name="prep",
    )

    squares = []
    for iteration in range(ITERS):
        part_eps = eps_part(x, bext, a_all, c_all, wfp, lat)
        got = lax.all_to_all(part_eps.reshape(members, mine, lanes), HOOD, 0, 0, tiled=True)
        if iteration < ITERS - 1:
            states, send, square = vmem_call(
                functools.partial(glue_body, lat, frames, cores),
                (
                    jax.ShapeDtypeStruct(states.shape, F32),
                    jax.ShapeDtypeStruct((members, mine, lanes), BF16),
                    jax.ShapeDtypeStruct((mine, lanes), F32),
                ),
                got,
                states,
                noise,
                base,
                fblk,
                coef,
                name="advance",
            )
            squares.append(square)
            x = lax.all_to_all(send, HOOD, 0, 0, tiled=True).reshape(tokens, lanes)
        else:
            send = smem_first(
                functools.partial(last_body, lat, frames, cores),
                jax.ShapeDtypeStruct((members, mine // 2, lanes), F32),
                where,
                got,
                states,
                noise,
                base,
                fblk,
                coef,
                *squares,
                name="last",
            )
    ended = lax.all_to_all(send, HOOD, 0, 0, tiled=True)
    trajectory, norms = smem_first(
        functools.partial(end_body, lat, frames, cores, float(step_n * lat * tokens)),
        (
            jax.ShapeDtypeStruct((lat, row_count), F32),
            jax.ShapeDtypeStruct((mine // 2, lanes), F32),
        ),
        where,
        ended,
        name="end",
    )
    return trajectory[None], norms[0, :ITERS]


def solution(mesh):
    names = ("parts", "zhi", "zlo", "frame", "head")
    sizes = mesh.shape
    devices = mesh.devices.reshape(
        sizes["parts"], sizes["step"] // ZLO, ZLO, sizes["frame"], sizes["head"]
    )
    return jax.shard_map(
        local,
        mesh=Mesh(devices, names),
        in_specs=(
            P("parts", "frame"),
            P("frame", None),
            P(),
            P(STEP),
            P(STEP),
            P(),
            P(),
            P(),
            P(),
            P(STEP, None, "head"),
            P(STEP, "head"),
            P(),
        ),
        out_specs=(P(STEP, "parts", "frame"), P("parts")),
        check_vma=False,
    )
```

```python
import functools
import math

import jax
import jax.numpy as jnp
from jax import lax
from jax.experimental import pallas as pl
from jax.experimental.pallas import tpu as pltpu
from jax.sharding import Mesh
from jax.sharding import PartitionSpec as P

HDIM = 72
ITERS = 4
ZLO = 4
GRANT = 16 * 1024 * 1024
F32 = jnp.float32
BF16 = jnp.bfloat16
STEP = ("zhi", "zlo")
HOOD = ("frame", "zlo", "head")


def chosen(pieces, index):
    out = pieces[0]
    for at, piece in enumerate(pieces[1:], 1):
        out = jnp.where(index == at, piece, out)
    return out


def vmem_call(body, out_shape, *args, scratch=(), flops=0, name=None):
    spec = pl.BlockSpec(memory_space=pltpu.VMEM)
    return pl.pallas_call(
        body,
        out_shape=out_shape,
        in_specs=[spec] * len(args),
        out_specs=jax.tree.map(lambda _: spec, out_shape),
        scratch_shapes=list(scratch),
        cost_estimate=pl.CostEstimate(flops=flops, bytes_accessed=0, transcendentals=0),
        compiler_params=pltpu.CompilerParams(vmem_limit_bytes=GRANT),
        name=name,
    )(*args)


def eps_body(heads, steps, lat, x_ref, bext_ref, a_ref, c_ref, wfp_ref, out_ref, xs, es, qs, ks, vs, os, s0, s1, m0, m1):
    cols = heads * HDIM
    tokens = x_ref.shape[0]
    xs[...] = x_ref[...].astype(F32).T
    scale = math.log2(math.e) / math.sqrt(HDIM)
    eight = lax.broadcasted_iota(jnp.int32, (steps, tokens), 0)
    blank = jnp.zeros((a_ref.shape[1] - 3 * (lat + steps), tokens), F32)
    ones8 = jnp.ones((8, tokens), F32)
    held, tops = (s0, s1), (m0, m1)

    lanes_pad = 128

    def project(step, carry):
        rows = pl.ds(pl.multiple_of(step * lat, lat), lat)
        x = xs[rows, :]
        pick = jnp.where(eight == step, 1.0, 0.0)
        xcat = jnp.concatenate([x, x, x, pick, pick, pick, blank], axis=0).astype(BF16)
        mixed = jnp.dot(a_ref[...], xcat, preferred_element_type=F32) + bext_ref[...]
        quad = mixed[3 * cols :, :]
        square = jnp.sum(x * quad, axis=0, keepdims=True) + c_ref[pl.ds(step, 1), :]
        rate = lax.rsqrt(jnp.maximum(square, 0.0) + 1e-06)
        for head in range(heads):
            q, k, v = (
                mixed[part * cols + head * HDIM : part * cols + (head + 1) * HDIM, :]
                for part in range(3)
            )
            qs[step, head] = (q * (rate * scale)).astype(BF16)
            ks[step, head] = (jnp.concatenate([k * rate, jnp.zeros((lanes_pad - HDIM, tokens), F32)], axis=0).T).astype(BF16)
            vs[step, head] = jnp.concatenate([v * rate, ones8], axis=0).astype(BF16)
        return carry

    lax.fori_loop(0, steps, project, 0, unroll=True)

    def score(step, head):
        s = jnp.dot(ks[step, head][:, :HDIM], qs[step, head], preferred_element_type=F32)
        held[head % 2][...] = s
        tops[head % 2][...] = jnp.max(s, axis=0, keepdims=True)

    def weigh(step, head):
        e = jnp.exp2(held[head % 2][...] - tops[head % 2][...]).astype(BF16)
        os[step, head] = jnp.dot(vs[step, head], e, preferred_element_type=F32)

    score(0, 0)

    def attend(step, carry):
        for head in range(heads):
            if head + 1 < heads:
                score(step, head + 1)
            else:
                score(jnp.minimum(step + 1, steps - 1), 0)
            weigh(step, head)
        return carry

    lax.fori_loop(0, steps, attend, 0, unroll=2)

    for step in range(steps):
        outs = []
        for head in range(heads):
            o = os[step, head]
            outs.append(o[:HDIM, :] * (1.0 / o[HDIM : HDIM + 1, :]))
        o = jnp.concatenate(outs, axis=0).astype(BF16)
        part = jnp.dot(wfp_ref[...], o, preferred_element_type=F32)
        es[step * lat : (step + 1) * lat, :] = part[:lat, :] + part[lat:, :]
    out_ref[...] = es[...].T.astype(BF16)


def eps_part(x, bext, a_all, c_all, wfp, lat):
    steps = c_all.shape[0]
    tokens = x.shape[0]
    heads = wfp.shape[1] // HDIM
    flops = 2 * steps * tokens * (bext.shape[0] * 64 + heads * tokens * 160)
    return vmem_call(
        functools.partial(eps_body, heads, steps, lat),
        jax.ShapeDtypeStruct((tokens, steps * lat), BF16),
        x,
        bext,
        a_all,
        c_all,
        wfp,
        scratch=(
            pltpu.VMEM((steps * lat, tokens), F32),
            pltpu.VMEM((steps * lat, tokens), F32),
            pltpu.VMEM((steps, heads, HDIM, tokens), BF16),
            pltpu.VMEM((steps, heads, tokens, 128), BF16),
            pltpu.VMEM((steps, heads, HDIM + 8, tokens), BF16),
            pltpu.VMEM((steps, heads, HDIM + 8, tokens), F32),
            pltpu.VMEM((tokens, tokens), F32),
            pltpu.VMEM((tokens, tokens), F32),
            pltpu.VMEM((1, tokens), F32),
            pltpu.VMEM((1, tokens), F32),
        ),
        flops=flops,
        name="eps_part",
    )


def advance(lat, frames, cores, got_ref, x_ref, noise_ref, base_ref, fblk_ref, coef_ref):
    groups, rows, lanes = x_ref.shape
    lane = lax.broadcasted_iota(jnp.int32, (rows, lanes), 1)
    before = jnp.zeros((rows, lanes), F32)
    drifts, states = [], []
    square = jnp.zeros((rows, lanes), F32)
    for group in range(groups):
        old = x_ref[group]
        total = base_ref[group]
        for frame in range(frames):
            for core in range(cores):
                member = (frame * groups + group) * cores + core
                total = total + got_ref[member].astype(F32)
        xb = old.astype(BF16)
        total = total + jnp.dot(
            jnp.concatenate([xb, xb, xb], axis=1), fblk_ref[...], preferred_element_type=F32
        )
        drift = (
            coef_ref[pl.ds(group, 1), :] * old + coef_ref[pl.ds(groups + group, 1), :] * total
        )
        running = drift
        shift = lat
        while shift < lanes:
            running = running + jnp.where(lane >= shift, pltpu.roll(running, shift, 1), 0.0)
            shift *= 2
        own = jnp.where(lane >= lat, pltpu.roll(running, lat, 1), 0.0)
        new = noise_ref[...] + before + own
        last = jnp.where(lane >= lanes - lat, running, 0.0)
        shift = lanes // 2
        while shift >= lat:
            last = last + pltpu.roll(last, shift, 1)
            shift //= 2
        before = before + last
        change = new - old
        square = square + change * change
        drifts.append(drift)
        states.append(new)
    return drifts, states, square


def glue_body(lat, frames, cores, got_ref, x_ref, noise_ref, base_ref, fblk_ref, coef_ref,
              new_ref, send_ref, square_ref):
    _, states, square = advance(
        lat, frames, cores, got_ref, x_ref, noise_ref, base_ref, fblk_ref, coef_ref
    )
    square_ref[...] = square
    groups = len(states)
    for group, new in enumerate(states):
        new_ref[group] = new
        rounded = new.astype(BF16)
        for frame in range(frames):
            for core in range(cores):
                send_ref[(frame * groups + group) * cores + core] = rounded


def last_body(lat, frames, cores, where_ref, got_ref, x_ref, noise_ref, base_ref, fblk_ref,
              coef_ref, sq0_ref, sq1_ref, sq2_ref, send_ref):
    drifts, states, square = advance(
        lat, frames, cores, got_ref, x_ref, noise_ref, base_ref, fblk_ref, coef_ref
    )
    groups, rows, lanes = x_ref.shape
    half = rows // 2
    zhi = where_ref[0]
    width = groups * lat
    first = zhi * groups
    per_group = lanes // lat
    picked = chosen([s + d for s, d in zip(states, drifts)], first // per_group)
    offset = lax.rem(first, per_group) * lat
    lane = lax.broadcasted_iota(jnp.int32, (half, lanes), 1)
    turn = lax.rem(lanes - offset, lanes)
    top = pltpu.roll(picked[:half], turn, 1)
    bottom = pltpu.roll(picked[half:], lax.rem(turn + width, lanes), 1)
    piece = jnp.where(lane < width, top, bottom)
    sums = jnp.zeros((half, lanes), F32)
    inner = lax.rem(lane, lat)
    for at, sq in enumerate((sq0_ref[...], sq1_ref[...], sq2_ref[...], square)):
        sums = jnp.where(inner == at, jnp.sum(sq), sums)
    for group in range(groups):
        slot = (group + 1) % groups
        mixed = jnp.where(lane // lat == slot, sums, piece)
        for frame in range(frames):
            for core in range(cores):
                send_ref[(frame * groups + group) * cores + core] = mixed


def end_body(lat, frames, cores, cells, where_ref, got_ref, traj_ref, norm_ref):
    members, half, lanes = got_ref.shape
    groups = members // (frames * cores)
    frame, zlo = where_ref[1], where_ref[2]
    width = groups * lat
    everyone = got_ref[0]
    for member in range(1, members):
        everyone = everyone + got_ref[member]
    slot = lax.rem(zlo + 1, groups)
    sums = pltpu.roll(everyone, lax.rem(lanes - slot * lat, lanes), 1)
    norms = jnp.sqrt(sums[:1] / cells + 1e-06)
    for at in range(ITERS):
        norm_ref[at] = norms[0, at]
    rows = []
    back = lax.rem(lanes - zlo * lat, lanes)
    for own in range(groups * cores):
        piece = got_ref[frame * (groups * cores) + own]
        rows.append(pltpu.roll(piece, back, 1))
        rows.append(pltpu.roll(piece, lax.rem(back + lanes - width, lanes), 1))
    traj_ref[...] = jnp.concatenate(rows, axis=0).T[:lat, :]


def smem_first(body, out_shape, where, *args, scratch=(), grant=GRANT, scalars=(), name=None):
    spec = pl.BlockSpec(memory_space=pltpu.VMEM)
    out_specs = jax.tree.map(lambda _: spec, out_shape)
    for at in scalars:
        out_specs = (*out_specs[:at], pl.BlockSpec(memory_space=pltpu.SMEM), *out_specs[at + 1 :])
    return pl.pallas_call(
        body,
        out_shape=out_shape,
        in_specs=[pl.BlockSpec(memory_space=pltpu.SMEM)] + [spec] * len(args),
        out_specs=out_specs,
        scratch_shapes=list(scratch),
        compiler_params=pltpu.CompilerParams(vmem_limit_bytes=grant),
        name=name,
    )(where, *args)


def split_two(a):
    hi = a.astype(BF16)
    return hi, (a - hi.astype(F32)).astype(BF16)


def split_lanes(a, lat, steps):
    hi = a.astype(BF16).astype(F32)
    mid = (a - hi).astype(BF16).astype(F32)
    low = a - hi - mid
    lane = lax.broadcasted_iota(jnp.int32, a.shape, 1)
    first, second, third = 3 * lat, 3 * lat + steps, 3 * lat + 2 * steps
    is_hi = (lane < lat) | ((lane >= first) & (lane < second))
    is_mid = ((lane >= lat) & (lane < 2 * lat)) | ((lane >= second) & (lane < third))
    return jnp.where(is_hi, hi, jnp.where(is_mid, mid, low)).astype(BF16)


def prep_body(lat, cores, extra, where_ref, got_ref, all_ref, position_ref, start_ref, table_ref,
              gain_ref, keep_ref, rate_ref, w_in_ref, final_ref, bext_ref, a_ref, c_ref, base_ref, fblk_ref, coef_ref, noise_ref, state_ref, x_ref,
              temb_ref, turned_ref, w_ref, index_ref):
    zlo, core = where_ref[2], where_ref[3]
    frames = all_ref.shape[0]
    rows, model = position_ref.shape
    groups, mine, lanes = base_ref.shape
    steps = lanes // lat
    count = groups * steps
    inv = 1.0 / model
    nt = (((1,), (1,)), ((), ()))

    def nt_dot(a, b):
        return lax.dot_general(a, b, nt, preferred_element_type=F32)

    rows_d = model // count
    tall = rows_d // 2
    for source in range(count):
        got = got_ref[source].astype(F32)
        at = source * rows_d
        for part in range(3):
            w_ref[at : at + rows_d, part * lanes : (part + 1) * lanes] = got[
                part * rows_d : (part + 1) * rows_d
            ]
        side = got[3 * rows_d : 3 * rows_d + tall]
        w_ref[at : at + tall, 3 * lanes :] = side
        w_ref[at + tall : at + rows_d, 3 * lanes :] = jnp.concatenate(
            [side[:, 3 * extra :], side[:, : 3 * extra]], axis=1
        )
        index_ref[source : source + 1] = got[3 * rows_d + tall : 3 * rows_d + tall + 1]

    spots = lax.broadcasted_iota(jnp.int32, (count, table_ref.shape[0]), 1).astype(F32)
    pick_time = jnp.where(index_ref[:, 0:1] == spots, 1.0, 0.0).astype(BF16)
    pick_sched = jnp.where(index_ref[:, 1:2] == spots, 1.0, 0.0)
    temb_all = jnp.dot(pick_time, table_ref[...], preferred_element_type=F32)
    temb_ref[...] = temb_all
    temb = temb_ref[pl.ds(pl.multiple_of(zlo * steps, steps), steps), :]
    lane = lax.broadcasted_iota(jnp.int32, (count, lanes), 1)
    own = lax.broadcasted_iota(jnp.int32, (count, lanes), 0)
    here = (lane // lat) == lax.rem(own, steps)

    def spread(a):
        return jnp.sum(jnp.where(here, a, 0.0).reshape(groups, steps, lanes), axis=1)

    keep = jnp.sum(pick_sched * keep_ref[...], axis=1, keepdims=True)
    rate = jnp.sum(pick_sched * rate_ref[...], axis=1, keepdims=True)
    coef_ref[:groups] = spread(jnp.broadcast_to(keep, (count, lanes)))
    coef_ref[groups:] = spread(jnp.broadcast_to(rate, (count, lanes)))

    final = final_ref[...].astype(F32)
    final = jnp.concatenate([final] * steps, axis=0).astype(BF16)
    w_in = w_in_ref[...].astype(F32)
    w_in_all = jnp.concatenate([w_in] * steps, axis=0).astype(BF16)
    mixed = nt_dot(w_in_all, final)
    square_lane = lax.broadcasted_iota(jnp.int32, (lanes, lanes), 1) // lat
    square_row = lax.broadcasted_iota(jnp.int32, (lanes, lanes), 0) // lat
    mixed = jnp.where(square_lane == square_row, mixed, 0.0)
    hi = mixed.astype(BF16)
    mid = (mixed - hi.astype(F32)).astype(BF16)
    fblk_ref[:lanes] = hi
    fblk_ref[lanes : 2 * lanes] = mid
    fblk_ref[2 * lanes :] = (mixed - hi.astype(F32) - mid.astype(F32)).astype(BF16)
    at = pl.multiple_of((zlo * cores + core) * mine, mine)
    base_own = nt_dot(position_ref[pl.ds(at, mine), :], final)
    base_time = spread(nt_dot(temb_all.astype(BF16), final))
    for group in range(groups):
        base_ref[group] = base_own + base_time[group : group + 1, :]

    turned_ref[...] = jnp.concatenate([start_ref[...]] * steps, axis=0).T
    noise = turned_ref[pl.ds(at, mine), :]
    noise_ref[...] = noise
    for group in range(groups):
        state_ref[group] = noise
    for frame in range(frames):
        noise = all_ref[frame, rows:, :rows].astype(F32)
        x_ref[frame * rows : (frame + 1) * rows] = (
            jnp.concatenate([noise] * steps, axis=0).T.astype(BF16)
        )

    blank = jnp.zeros((lanes - 3 * (lat + steps), model), F32)
    thin = jnp.concatenate([w_in, w_in, w_in, temb, temb, temb, blank], axis=0)
    thin_bf = thin.astype(BF16)
    gain = jnp.concatenate([gain_ref[at : at + 1] for at in range(model // lanes)], axis=1)
    w = w_ref[...].astype(BF16)
    thin_hi, thin_lo = split_two(thin * gain)
    linear = jnp.dot(thin_hi, w, preferred_element_type=F32) + jnp.dot(
        thin_lo, w, preferred_element_type=F32
    )
    places = []
    for part in range(3):
        places += [(part * lanes, lanes), (3 * lanes + part * extra, extra)]
    row = 0
    turned = linear.T
    for start, size in places:
        a_ref[row : row + size] = split_lanes(turned[start : start + size], lat, steps)
        row += size
    gram = nt_dot(thin_bf[:lat], thin_bf)
    gram_lane = lax.broadcasted_iota(jnp.int32, gram.shape, 1)
    gram = gram * jnp.where(gram_lane < 3 * lat, inv, 2.0 * inv)
    a_ref[row:] = split_lanes(gram, lat, steps)
    temb_square = jnp.sum(temb * temb, axis=1, keepdims=True)
    for frame in range(frames):
        there = pl.ds(frame * rows, rows)
        tokens_bf = all_ref[frame, :rows, :]
        wide = tokens_bf.astype(F32)
        wide_hi, wide_lo = split_two(wide * gain)
        linear = (
            jnp.dot(wide_hi, w, preferred_element_type=F32)
            + jnp.dot(wide_lo, w, preferred_element_type=F32)
        ).T
        row = 0
        for start, size in places:
            bext_ref[row : row + size, frame * rows : (frame + 1) * rows] = linear[
                start : start + size
            ]
            row += size
        gram = nt_dot(thin_bf, tokens_bf)
        bext_ref[row:, frame * rows : (frame + 1) * rows] = gram[:lat] * (2.0 * inv)
        square = wide * wide
        folded = square[:, :lanes]
        for chunk in range(1, model // lanes):
            folded = folded + square[:, chunk * lanes : (chunk + 1) * lanes]
        square = jnp.sum(folded.T, axis=0, keepdims=True)
        c_ref[:, frame * rows : (frame + 1) * rows] = inv * (
            square + 2.0 * gram[3 * lat : 3 * lat + steps] + temb_square
        )


def exact_pick(values, wanted):
    return jnp.dot(values, jnp.where(wanted, 1.0, 0.0).astype(BF16), preferred_element_type=F32)


def pack_body(extra, where_ref, qkv_ref, proj_ref, final_ref, start_ref, position_ref,
              mix_ref, frame_ref, main_ref, rows_ref, half_ref):
    frame, step = where_ref[1], where_ref[4]
    lat, rows = start_ref.shape
    rows_d, width = proj_ref.shape
    frames, parts = frame_ref.shape[0], mix_ref.shape[0]
    lanes = main_ref.shape[1]
    cols = mix_ref.shape[2]
    tall = rows_d // 2

    column = lax.broadcasted_iota(jnp.int32, (width, 2 * lanes), 0) - frame * cols
    lane = lax.broadcasted_iota(jnp.int32, (width, 2 * lanes), 1)
    both = column == lane
    model = final_ref.shape[1]
    feature = lax.broadcasted_iota(jnp.int32, (model, lanes), 0) - step * rows_d
    final = exact_pick(final_ref[...], feature == lax.broadcasted_iota(jnp.int32, (model, lanes), 1))
    proj = exact_pick(proj_ref[...], both)
    blank = jnp.zeros((lanes - rows_d, 2 * lanes), F32)
    proj = jnp.concatenate([proj, blank], axis=0).astype(BF16)
    feature_lane = lax.broadcasted_iota(jnp.int32, final.shape, 1)
    final = jnp.where(feature_lane < rows_d, final, 0.0).astype(BF16)
    mix = jnp.dot(final, proj, preferred_element_type=F32)
    each = lat // parts
    for part in range(parts):
        mix_ref[part] = mix[part * each : (part + 1) * each, :cols]

    noise = jnp.concatenate(
        [start_ref[...], jnp.zeros((lat, model - rows), F32)], axis=1
    ).astype(BF16)
    for at in range(frames):
        frame_ref[at, :rows] = position_ref[...]
        frame_ref[at, rows:] = noise

    side = jnp.zeros((rows_d, 2 * lanes), F32)
    for part in range(3):
        weights = qkv_ref[part]
        rows_ref[part * rows_d : (part + 1) * rows_d, :] = exact_pick(weights, both)[:, :lanes]
        shifted = lane - part * extra
        first = (column - lanes == shifted) & (shifted >= 0) & (shifted < extra)
        shifted = lane - lanes - (3 + part) * extra
        second = (column - lanes == shifted) & (shifted >= 0) & (shifted < extra)
        side = side + exact_pick(weights, first | second)
    half_ref[...] = side[:, lanes:]
    rows_ref[3 * rows_d : 3 * rows_d + tall, :] = side[:tall, :lanes] + half_ref[tall:, :]
    spot = lax.broadcasted_iota(jnp.int32, (1, lanes), 1)
    times = where_ref[5].astype(F32)
    plans = where_ref[6].astype(F32)
    rows_ref[3 * rows_d + tall : 3 * rows_d + tall + 1, :] = jnp.where(
        spot == 0, times, jnp.where(spot == 1, plans, 0.0)
    )
    main_ref[...] = rows_ref[...][: main_ref.shape[0], :].astype(BF16)


def local(
    start_noise,
    position,
    time_table,
    time_index,
    sched_index,
    coef_keep,
    coef_noise,
    w_in,
    norm_gain,
    w_qkv,
    w_proj,
    w_final,
):
    lat, row_count = start_noise.shape
    rows_d = w_qkv.shape[0]
    model = position.shape[1]
    frames, cores = lax.axis_size("frame"), lax.axis_size("head")
    zlo_n, zhi_n = lax.axis_size("zlo"), lax.axis_size("zhi")
    step_n = zlo_n * zhi_n
    steps = step_n // zlo_n
    tokens = row_count * frames
    cols = w_qkv.shape[2] // frames
    heads = cols // HDIM
    members = frames * zlo_n * cores
    mine = tokens // members
    lanes = steps * lat
    frame, zlo, zhi, core = (lax.axis_index(a) for a in ("frame", "zlo", "zhi", "head"))
    step = zhi * zlo_n + zlo

    where = jnp.concatenate(
        [jnp.stack([zhi, frame, zlo, core, step]).astype(jnp.int32), time_index, sched_index]
    )
    tall = rows_d // 2
    extra = cols - lanes
    pieces = cols // tall
    payload_rows = 3 * rows_d + tall + 1
    mix, frame_load, payload = smem_first(
        functools.partial(pack_body, extra),
        (
            jax.ShapeDtypeStruct((zlo_n, lat // zlo_n, cols), F32),
            jax.ShapeDtypeStruct((frames, row_count + lat, model), BF16),
            jax.ShapeDtypeStruct((payload_rows, lanes), BF16),
        ),
        where,
        w_qkv.transpose(1, 0, 2),
        w_proj,
        w_final,
        start_noise,
        position,
        scratch=(pltpu.VMEM((payload_rows + 1, lanes), F32), pltpu.VMEM((rows_d, lanes), F32)),
        grant=None,
        name="pack",
    )

    mix = jnp.sum(lax.all_to_all(mix, "zlo", 0, 0, tiled=True), axis=0)
    mix = mix.reshape(lat // zlo_n, pieces, tall).transpose(2, 1, 0).reshape(tall, -1)
    payload = payload + jnp.pad(
        mix.astype(BF16), ((3 * rows_d, 1), (6 * extra, lanes - 6 * extra - mix.shape[1]))
    )

    frame_all = lax.all_to_all(frame_load, "frame", 0, 0, tiled=True)

    gathered = lax.all_gather(payload, STEP, axis=0)

    sides = gathered[:, 3 * rows_d : 3 * rows_d + tall]
    part = lat // zlo_n
    mixes = sides[:, :, 6 * extra :].astype(F32).reshape(zhi_n, zlo_n, tall, pieces, part)
    mixes = jnp.sum(mixes, axis=0).transpose(0, 3, 2, 1).reshape(lat, cols)
    mix_hi = lax.reduce_precision(mixes, 8, 7)
    wfp = jnp.concatenate([mix_hi, mixes - mix_hi], axis=0).astype(BF16)
    bext, a_all, c_all, base, fblk, coef, noise, states, x = smem_first(
        functools.partial(prep_body, lat, cores, extra),
        (
            jax.ShapeDtypeStruct((3 * cols + lat, tokens), F32),
            jax.ShapeDtypeStruct((3 * cols + lat, lanes), BF16),
            jax.ShapeDtypeStruct((steps, tokens), F32),
            jax.ShapeDtypeStruct((zlo_n, mine, lanes), F32),
            jax.ShapeDtypeStruct((3 * lanes, lanes), BF16),
            jax.ShapeDtypeStruct((2 * zlo_n, lanes), F32),
            jax.ShapeDtypeStruct((mine, lanes), F32),
            jax.ShapeDtypeStruct((zlo_n, mine, lanes), F32),
            jax.ShapeDtypeStruct((tokens, lanes), BF16),
        ),
        where,
        gathered,
        frame_all,
        position,
        start_noise,
        time_table,
        norm_gain.reshape(-1, lanes),
        coef_keep[None],
        coef_noise[None],
        w_in,
        w_final,
        scratch=(
            pltpu.VMEM((step_n, model), F32),
            pltpu.VMEM((row_count, lanes), F32),
            pltpu.VMEM((step_n * rows_d, 4 * lanes), F32),
            pltpu.VMEM((step_n, lanes), F32),
        ),
        name="prep",
    )

    squares = []
    for iteration in range(ITERS):
        part_eps = eps_part(x, bext, a_all, c_all, wfp, lat)
        got = lax.all_to_all(part_eps.reshape(members, mine, lanes), HOOD, 0, 0, tiled=True)
        if iteration < ITERS - 1:
            states, send, square = vmem_call(
                functools.partial(glue_body, lat, frames, cores),
                (
                    jax.ShapeDtypeStruct(states.shape, F32),
                    jax.ShapeDtypeStruct((members, mine, lanes), BF16),
                    jax.ShapeDtypeStruct((mine, lanes), F32),
                ),
                got,
                states,
                noise,
                base,
                fblk,
                coef,
                name="advance",
            )
            squares.append(square)
            x = lax.all_to_all(send, HOOD, 0, 0, tiled=True).reshape(tokens, lanes)
        else:
            send = smem_first(
                functools.partial(last_body, lat, frames, cores),
                jax.ShapeDtypeStruct((members, mine // 2, lanes), F32),
                where,
                got,
                states,
                noise,
                base,
                fblk,
                coef,
                *squares,
                name="last",
            )
    ended = lax.all_to_all(send, HOOD, 0, 0, tiled=True)
    trajectory, norms = smem_first(
        functools.partial(end_body, lat, frames, cores, float(step_n * lat * tokens)),
        (
            jax.ShapeDtypeStruct((lat, row_count), F32),
            jax.ShapeDtypeStruct((ITERS,), F32),
        ),
        where,
        ended,
        scalars=(1,),
        name="end",
    )
    return trajectory[None], norms


def solution(mesh):
    names = ("parts", "zhi", "zlo", "frame", "head")
    sizes = mesh.shape
    devices = mesh.devices.reshape(
        sizes["parts"], sizes["step"] // ZLO, ZLO, sizes["frame"], sizes["head"]
    )
    return jax.shard_map(
        local,
        mesh=Mesh(devices, names),
        in_specs=(
            P("parts", "frame"),
            P("frame", None),
            P(),
            P(STEP),
            P(STEP),
            P(),
            P(),
            P(),
            P(),
            P(STEP, None, "head"),
            P(STEP, "head"),
            P(),
        ),
        out_specs=(P(STEP, "parts", "frame"), P("parts")),
        check_vma=False,
    )
```

```python
import functools
import math

import jax
import jax.numpy as jnp
from jax import lax
from jax.experimental import pallas as pl
from jax.experimental.pallas import tpu as pltpu
from jax.sharding import Mesh
from jax.sharding import PartitionSpec as P

HDIM = 72
ITERS = 4
ZLO = 4
GRANT = 16 * 1024 * 1024
F32 = jnp.float32
BF16 = jnp.bfloat16
STEP = ("zhi", "zlo")
HOOD = ("frame", "zlo", "head")


def chosen(pieces, index):
    out = pieces[0]
    for at, piece in enumerate(pieces[1:], 1):
        out = jnp.where(index == at, piece, out)
    return out


def vmem_call(body, out_shape, *args, scratch=(), flops=0, name=None):
    spec = pl.BlockSpec(memory_space=pltpu.VMEM)
    return pl.pallas_call(
        body,
        out_shape=out_shape,
        in_specs=[spec] * len(args),
        out_specs=jax.tree.map(lambda _: spec, out_shape),
        scratch_shapes=list(scratch),
        cost_estimate=pl.CostEstimate(flops=flops, bytes_accessed=0, transcendentals=0),
        compiler_params=pltpu.CompilerParams(vmem_limit_bytes=GRANT),
        name=name,
    )(*args)


def eps_body(heads, steps, lat, x_ref, bext_ref, a_ref, c_ref, wfp_ref, out_ref, xs, es, qs, ks, vs, os, s0, s1, m0, m1):
    cols = heads * HDIM
    tokens = x_ref.shape[0]
    xs[...] = x_ref[...].astype(F32).T
    scale = math.log2(math.e) / math.sqrt(HDIM)
    eight = lax.broadcasted_iota(jnp.int32, (steps, tokens), 0)
    blank = jnp.zeros((a_ref.shape[1] - 3 * (lat + steps), tokens), F32)
    ones8 = jnp.ones((8, tokens), F32)
    held, tops = (s0, s1), (m0, m1)

    lanes_pad = 128

    def project(step, carry):
        rows = pl.ds(pl.multiple_of(step * lat, lat), lat)
        x = xs[rows, :]
        pick = jnp.where(eight == step, 1.0, 0.0)
        xcat = jnp.concatenate([x, x, x, pick, pick, pick, blank], axis=0).astype(BF16)
        mixed = jnp.dot(a_ref[...], xcat, preferred_element_type=F32) + bext_ref[...]
        quad = mixed[3 * cols :, :]
        square = jnp.sum(x * quad, axis=0, keepdims=True) + c_ref[pl.ds(step, 1), :]
        rate = lax.rsqrt(jnp.maximum(square, 0.0) + 1e-06)
        for head in range(heads):
            q, k, v = (
                mixed[part * cols + head * HDIM : part * cols + (head + 1) * HDIM, :]
                for part in range(3)
            )
            qs[step, head] = (q * (rate * scale)).astype(BF16)
            ks[step, head] = (jnp.concatenate([k * rate, jnp.zeros((lanes_pad - HDIM, tokens), F32)], axis=0).T).astype(BF16)
            vs[step, head] = jnp.concatenate([v * rate, ones8], axis=0).astype(BF16)
        return carry

    lax.fori_loop(0, steps, project, 0, unroll=True)

    def score(step, head):
        s = jnp.dot(ks[step, head][:, :HDIM], qs[step, head], preferred_element_type=F32)
        held[head % 2][...] = s
        tops[head % 2][...] = jnp.max(s, axis=0, keepdims=True)

    def weigh(step, head):
        e = jnp.exp2(held[head % 2][...] - tops[head % 2][...]).astype(BF16)
        os[step, head] = jnp.dot(vs[step, head], e, preferred_element_type=F32)

    score(0, 0)

    def attend(step, carry):
        for head in range(heads):
            if head + 1 < heads:
                score(step, head + 1)
            else:
                score(jnp.minimum(step + 1, steps - 1), 0)
            weigh(step, head)
        return carry

    lax.fori_loop(0, steps, attend, 0, unroll=2)

    for step in range(steps):
        outs = []
        for head in range(heads):
            o = os[step, head]
            outs.append(o[:HDIM, :] * (1.0 / o[HDIM : HDIM + 1, :]))
        o = jnp.concatenate(outs, axis=0).astype(BF16)
        part = jnp.dot(wfp_ref[...], o, preferred_element_type=F32)
        es[step * lat : (step + 1) * lat, :] = part[:lat, :] + part[lat:, :]
    out_ref[...] = es[...].T.astype(BF16)


def eps_part(x, bext, a_all, c_all, wfp, lat):
    steps = c_all.shape[0]
    tokens = x.shape[0]
    heads = wfp.shape[1] // HDIM
    flops = 2 * steps * tokens * (bext.shape[0] * 64 + heads * tokens * 160)
    return vmem_call(
        functools.partial(eps_body, heads, steps, lat),
        jax.ShapeDtypeStruct((tokens, steps * lat), BF16),
        x,
        bext,
        a_all,
        c_all,
        wfp,
        scratch=(
            pltpu.VMEM((steps * lat, tokens), F32),
            pltpu.VMEM((steps * lat, tokens), F32),
            pltpu.VMEM((steps, heads, HDIM, tokens), BF16),
            pltpu.VMEM((steps, heads, tokens, 128), BF16),
            pltpu.VMEM((steps, heads, HDIM + 8, tokens), BF16),
            pltpu.VMEM((steps, heads, HDIM + 8, tokens), F32),
            pltpu.VMEM((tokens, tokens), F32),
            pltpu.VMEM((tokens, tokens), F32),
            pltpu.VMEM((1, tokens), F32),
            pltpu.VMEM((1, tokens), F32),
        ),
        flops=flops,
        name="eps_part",
    )


def advance(lat, frames, cores, got_ref, x_ref, noise_ref, base_ref, fblk_ref, coef_ref):
    groups, rows, lanes = x_ref.shape
    lane = lax.broadcasted_iota(jnp.int32, (rows, lanes), 1)
    before = jnp.zeros((rows, lanes), F32)
    drifts, states = [], []
    square = jnp.zeros((rows, lanes), F32)
    for group in range(groups):
        old = x_ref[group]
        total = base_ref[group]
        for frame in range(frames):
            for core in range(cores):
                member = (frame * groups + group) * cores + core
                total = total + got_ref[member].astype(F32)
        xb = old.astype(BF16)
        total = total + jnp.dot(
            jnp.concatenate([xb, xb, xb], axis=1), fblk_ref[...], preferred_element_type=F32
        )
        drift = (
            coef_ref[pl.ds(group, 1), :] * old + coef_ref[pl.ds(groups + group, 1), :] * total
        )
        running = drift
        shift = lat
        while shift < lanes:
            running = running + jnp.where(lane >= shift, pltpu.roll(running, shift, 1), 0.0)
            shift *= 2
        own = jnp.where(lane >= lat, pltpu.roll(running, lat, 1), 0.0)
        new = noise_ref[...] + before + own
        last = jnp.where(lane >= lanes - lat, running, 0.0)
        shift = lanes // 2
        while shift >= lat:
            last = last + pltpu.roll(last, shift, 1)
            shift //= 2
        before = before + last
        change = new - old
        square = square + change * change
        drifts.append(drift)
        states.append(new)
    return drifts, states, square


def glue_body(lat, frames, cores, got_ref, x_ref, noise_ref, base_ref, fblk_ref, coef_ref,
              new_ref, send_ref, square_ref):
    _, states, square = advance(
        lat, frames, cores, got_ref, x_ref, noise_ref, base_ref, fblk_ref, coef_ref
    )
    square_ref[...] = square
    groups = len(states)
    for group, new in enumerate(states):
        new_ref[group] = new
        rounded = new.astype(BF16)
        for frame in range(frames):
            for core in range(cores):
                send_ref[(frame * groups + group) * cores + core] = rounded


def last_body(lat, frames, cores, got_ref, x_ref, noise_ref, base_ref, fblk_ref,
              coef_ref, sq0_ref, sq1_ref, sq2_ref, send_ref):
    drifts, states, square = advance(
        lat, frames, cores, got_ref, x_ref, noise_ref, base_ref, fblk_ref, coef_ref
    )
    groups, rows, lanes = x_ref.shape
    half = rows // 2
    zhi = lax.axis_index("zhi")
    width = groups * lat
    first = zhi * groups
    per_group = lanes // lat
    picked = chosen([s + d for s, d in zip(states, drifts)], first // per_group)
    offset = lax.rem(first, per_group) * lat
    lane = lax.broadcasted_iota(jnp.int32, (half, lanes), 1)
    turn = lax.rem(lanes - offset, lanes)
    top = pltpu.roll(picked[:half], turn, 1)
    bottom = pltpu.roll(picked[half:], lax.rem(turn + width, lanes), 1)
    piece = jnp.where(lane < width, top, bottom)
    sums = jnp.zeros((half, lanes), F32)
    inner = lax.rem(lane, lat)
    for at, sq in enumerate((sq0_ref[...], sq1_ref[...], sq2_ref[...], square)):
        sums = jnp.where(inner == at, jnp.sum(sq), sums)
    for group in range(groups):
        slot = (group + 1) % groups
        mixed = jnp.where(lane // lat == slot, sums, piece)
        for frame in range(frames):
            for core in range(cores):
                send_ref[(frame * groups + group) * cores + core] = mixed


def end_body(lat, frames, cores, cells, got_ref, traj_ref, norm_ref):
    members, half, lanes = got_ref.shape
    groups = members // (frames * cores)
    frame, zlo = lax.axis_index("frame"), lax.axis_index("zlo")
    width = groups * lat
    everyone = got_ref[0]
    for member in range(1, members):
        everyone = everyone + got_ref[member]
    slot = lax.rem(zlo + 1, groups)
    sums = pltpu.roll(everyone, lax.rem(lanes - slot * lat, lanes), 1)
    norms = jnp.sqrt(sums[:1] / cells + 1e-06)
    for at in range(ITERS):
        norm_ref[at] = norms[0, at]
    rows = []
    back = lax.rem(lanes - zlo * lat, lanes)
    for own in range(groups * cores):
        piece = got_ref[frame * (groups * cores) + own]
        rows.append(pltpu.roll(piece, back, 1))
        rows.append(pltpu.roll(piece, lax.rem(back + lanes - width, lanes), 1))
    traj_ref[...] = jnp.concatenate(rows, axis=0).T[:lat, :]


def smem_first(body, out_shape, *args, smem=0, scratch=(), grant=GRANT, scalars=(), flops=0, name=None):
    spec = pl.BlockSpec(memory_space=pltpu.VMEM)
    held = pl.BlockSpec(memory_space=pltpu.SMEM)
    out_specs = jax.tree.map(lambda _: spec, out_shape)
    for at in scalars:
        out_specs = (*out_specs[:at], held, *out_specs[at + 1 :])
    return pl.pallas_call(
        body,
        out_shape=out_shape,
        in_specs=[held] * smem + [spec] * (len(args) - smem),
        out_specs=out_specs,
        scratch_shapes=list(scratch),
        cost_estimate=pl.CostEstimate(flops=flops, bytes_accessed=0, transcendentals=0),
        compiler_params=pltpu.CompilerParams(vmem_limit_bytes=grant),
        name=name,
    )(*args)


def split_two(a):
    hi = a.astype(BF16)
    return hi, (a - hi.astype(F32)).astype(BF16)


def split_lanes(a, lat, steps):
    hi = a.astype(BF16).astype(F32)
    mid = (a - hi).astype(BF16).astype(F32)
    low = a - hi - mid
    lane = lax.broadcasted_iota(jnp.int32, a.shape, 1)
    first, second, third = 3 * lat, 3 * lat + steps, 3 * lat + 2 * steps
    is_hi = (lane < lat) | ((lane >= first) & (lane < second))
    is_mid = ((lane >= lat) & (lane < 2 * lat)) | ((lane >= second) & (lane < third))
    return jnp.where(is_hi, hi, jnp.where(is_mid, mid, low)).astype(BF16)


def prep_body(lat, cores, extra, got_ref, all_ref, position_ref, start_ref, table_ref,
              gain_ref, keep_ref, rate_ref, w_in_ref, final_ref, bext_ref, a_ref, c_ref, base_ref, fblk_ref, coef_ref, noise_ref, state_ref, x_ref,
              temb_ref, turned_ref, w_ref, index_ref):
    zlo, core = lax.axis_index("zlo"), lax.axis_index("head")
    frames = all_ref.shape[0]
    rows, model = position_ref.shape
    groups, mine, lanes = base_ref.shape
    steps = lanes // lat
    count = groups * steps
    inv = 1.0 / model
    nt = (((1,), (1,)), ((), ()))

    def nt_dot(a, b):
        return lax.dot_general(a, b, nt, preferred_element_type=F32)

    rows_d = model // count
    tall = rows_d // 2
    for source in range(count):
        got = got_ref[source].astype(F32)
        at = source * rows_d
        for part in range(3):
            w_ref[at : at + rows_d, part * lanes : (part + 1) * lanes] = got[
                part * rows_d : (part + 1) * rows_d
            ]
        side = got[3 * rows_d : 3 * rows_d + tall]
        w_ref[at : at + tall, 3 * lanes :] = side
        w_ref[at + tall : at + rows_d, 3 * lanes :] = jnp.concatenate(
            [side[:, 3 * extra :], side[:, : 3 * extra]], axis=1
        )
        index_ref[source : source + 1] = got[3 * rows_d + tall : 3 * rows_d + tall + 1]

    spots = lax.broadcasted_iota(jnp.int32, (count, table_ref.shape[0]), 1).astype(F32)
    pick_time = jnp.where(index_ref[:, 0:1] == spots, 1.0, 0.0).astype(BF16)
    pick_sched = jnp.where(index_ref[:, 1:2] == spots, 1.0, 0.0)
    temb_all = jnp.dot(pick_time, table_ref[...], preferred_element_type=F32)
    temb_ref[...] = temb_all
    temb = temb_ref[pl.ds(pl.multiple_of(zlo * steps, steps), steps), :]
    lane = lax.broadcasted_iota(jnp.int32, (count, lanes), 1)
    own = lax.broadcasted_iota(jnp.int32, (count, lanes), 0)
    here = (lane // lat) == lax.rem(own, steps)

    def spread(a):
        return jnp.sum(jnp.where(here, a, 0.0).reshape(groups, steps, lanes), axis=1)

    keep = jnp.sum(pick_sched * keep_ref[...], axis=1, keepdims=True)
    rate = jnp.sum(pick_sched * rate_ref[...], axis=1, keepdims=True)
    coef_ref[:groups] = spread(jnp.broadcast_to(keep, (count, lanes)))
    coef_ref[groups:] = spread(jnp.broadcast_to(rate, (count, lanes)))

    final = final_ref[...].astype(F32)
    final = jnp.concatenate([final] * steps, axis=0).astype(BF16)
    w_in = w_in_ref[...].astype(F32)
    w_in_all = jnp.concatenate([w_in] * steps, axis=0).astype(BF16)
    mixed = nt_dot(w_in_all, final)
    square_lane = lax.broadcasted_iota(jnp.int32, (lanes, lanes), 1) // lat
    square_row = lax.broadcasted_iota(jnp.int32, (lanes, lanes), 0) // lat
    mixed = jnp.where(square_lane == square_row, mixed, 0.0)
    hi = mixed.astype(BF16)
    mid = (mixed - hi.astype(F32)).astype(BF16)
    fblk_ref[:lanes] = hi
    fblk_ref[lanes : 2 * lanes] = mid
    fblk_ref[2 * lanes :] = (mixed - hi.astype(F32) - mid.astype(F32)).astype(BF16)
    at = pl.multiple_of((zlo * cores + core) * mine, mine)
    base_own = nt_dot(position_ref[pl.ds(at, mine), :], final)
    base_time = spread(nt_dot(temb_all.astype(BF16), final))
    for group in range(groups):
        base_ref[group] = base_own + base_time[group : group + 1, :]

    turned_ref[...] = jnp.concatenate([start_ref[...]] * steps, axis=0).T
    noise = turned_ref[pl.ds(at, mine), :]
    noise_ref[...] = noise
    for group in range(groups):
        state_ref[group] = noise
    for frame in range(frames):
        noise = all_ref[frame, rows:, :rows].astype(F32)
        x_ref[frame * rows : (frame + 1) * rows] = (
            jnp.concatenate([noise] * steps, axis=0).T.astype(BF16)
        )

    blank = jnp.zeros((lanes - 3 * (lat + steps), model), F32)
    thin = jnp.concatenate([w_in, w_in, w_in, temb, temb, temb, blank], axis=0)
    thin_bf = thin.astype(BF16)
    gain = jnp.concatenate([gain_ref[at : at + 1] for at in range(model // lanes)], axis=1)
    w = w_ref[...].astype(BF16)
    thin_hi, thin_lo = split_two(thin * gain)
    linear = jnp.dot(thin_hi, w, preferred_element_type=F32) + jnp.dot(
        thin_lo, w, preferred_element_type=F32
    )
    places = []
    for part in range(3):
        places += [(part * lanes, lanes), (3 * lanes + part * extra, extra)]
    row = 0
    turned = linear.T
    for start, size in places:
        a_ref[row : row + size] = split_lanes(turned[start : start + size], lat, steps)
        row += size
    gram = nt_dot(thin_bf[:lat], thin_bf)
    gram_lane = lax.broadcasted_iota(jnp.int32, gram.shape, 1)
    gram = gram * jnp.where(gram_lane < 3 * lat, inv, 2.0 * inv)
    a_ref[row:] = split_lanes(gram, lat, steps)
    temb_square = jnp.sum(temb * temb, axis=1, keepdims=True)
    for frame in range(frames):
        there = pl.ds(frame * rows, rows)
        tokens_bf = all_ref[frame, :rows, :]
        wide = tokens_bf.astype(F32)
        wide_hi, wide_lo = split_two(wide * gain)
        linear = (
            jnp.dot(wide_hi, w, preferred_element_type=F32)
            + jnp.dot(wide_lo, w, preferred_element_type=F32)
        ).T
        row = 0
        for start, size in places:
            bext_ref[row : row + size, frame * rows : (frame + 1) * rows] = linear[
                start : start + size
            ]
            row += size
        gram = nt_dot(thin_bf, tokens_bf)
        bext_ref[row:, frame * rows : (frame + 1) * rows] = gram[:lat] * (2.0 * inv)
        square = wide * wide
        folded = square[:, :lanes]
        for chunk in range(1, model // lanes):
            folded = folded + square[:, chunk * lanes : (chunk + 1) * lanes]
        square = jnp.sum(folded.T, axis=0, keepdims=True)
        c_ref[:, frame * rows : (frame + 1) * rows] = inv * (
            square + 2.0 * gram[3 * lat : 3 * lat + steps] + temb_square
        )


def exact_pick(values, wanted):
    return jnp.dot(values, jnp.where(wanted, 1.0, 0.0).astype(BF16), preferred_element_type=F32)


def mix_body(proj_ref, final_ref, mix_ref):
    frame = lax.axis_index("frame")
    step = lax.axis_index("zhi") * lax.axis_size("zlo") + lax.axis_index("zlo")
    lat, model = final_ref.shape
    rows_d, width = proj_ref.shape
    parts, each, cols = mix_ref.shape
    lanes = 128
    column = lax.broadcasted_iota(jnp.int32, (width, 2 * lanes), 0) - frame * cols
    both = column == lax.broadcasted_iota(jnp.int32, (width, 2 * lanes), 1)
    feature = lax.broadcasted_iota(jnp.int32, (model, lanes), 0) - step * rows_d
    final = exact_pick(final_ref[...], feature == lax.broadcasted_iota(jnp.int32, (model, lanes), 1))
    proj = exact_pick(proj_ref[...], both)
    blank = jnp.zeros((lanes - rows_d, 2 * lanes), F32)
    proj = jnp.concatenate([proj, blank], axis=0).astype(BF16)
    feature_lane = lax.broadcasted_iota(jnp.int32, final.shape, 1)
    final = jnp.where(feature_lane < rows_d, final, 0.0).astype(BF16)
    mix = jnp.dot(final, proj, preferred_element_type=F32)
    for part in range(parts):
        mix_ref[part] = mix[part * each : (part + 1) * each, :cols]


def pack_body(extra, cols, time_ref, plan_ref, qkv_ref, start_ref, position_ref,
              frame_ref, main_ref, rows_ref, half_ref):
    frame = lax.axis_index("frame")
    lat, rows = start_ref.shape
    rows_d, width = qkv_ref.shape[1:]
    frames = frame_ref.shape[0]
    lanes = main_ref.shape[1]
    tall = rows_d // 2

    column = lax.broadcasted_iota(jnp.int32, (width, 2 * lanes), 0) - frame * cols
    lane = lax.broadcasted_iota(jnp.int32, (width, 2 * lanes), 1)
    both = column == lane
    model = position_ref.shape[1]

    noise = jnp.concatenate(
        [start_ref[...], jnp.zeros((lat, model - rows), F32)], axis=1
    ).astype(BF16)
    for at in range(frames):
        frame_ref[at, :rows] = position_ref[...]
        frame_ref[at, rows:] = noise

    side = jnp.zeros((rows_d, 2 * lanes), F32)
    for part in range(3):
        weights = qkv_ref[part]
        rows_ref[part * rows_d : (part + 1) * rows_d, :] = exact_pick(weights, both)[:, :lanes]
        shifted = lane - part * extra
        first = (column - lanes == shifted) & (shifted >= 0) & (shifted < extra)
        shifted = lane - lanes - (3 + part) * extra
        second = (column - lanes == shifted) & (shifted >= 0) & (shifted < extra)
        side = side + exact_pick(weights, first | second)
    half_ref[...] = side[:, lanes:]
    rows_ref[3 * rows_d : 3 * rows_d + tall, :] = side[:tall, :lanes] + half_ref[tall:, :]
    spot = lax.broadcasted_iota(jnp.int32, (1, lanes), 1)
    times = time_ref[0].astype(F32)
    plans = plan_ref[0].astype(F32)
    rows_ref[3 * rows_d + tall : 3 * rows_d + tall + 1, :] = jnp.where(
        spot == 0, times, jnp.where(spot == 1, plans, 0.0)
    )
    main_ref[...] = rows_ref[...][: main_ref.shape[0], :].astype(BF16)


def local(
    start_noise,
    position,
    time_table,
    time_index,
    sched_index,
    coef_keep,
    coef_noise,
    w_in,
    norm_gain,
    w_qkv,
    w_proj,
    w_final,
):
    lat, row_count = start_noise.shape
    rows_d = w_qkv.shape[0]
    model = position.shape[1]
    frames, cores = lax.axis_size("frame"), lax.axis_size("head")
    zlo_n, zhi_n = lax.axis_size("zlo"), lax.axis_size("zhi")
    step_n = zlo_n * zhi_n
    steps = step_n // zlo_n
    tokens = row_count * frames
    cols = w_qkv.shape[2] // frames
    heads = cols // HDIM
    members = frames * zlo_n * cores
    mine = tokens // members
    lanes = steps * lat

    tall = rows_d // 2
    extra = cols - lanes
    pieces = cols // tall
    payload_rows = 3 * rows_d + tall + 1
    mix = smem_first(
        mix_body,
        jax.ShapeDtypeStruct((zlo_n, lat // zlo_n, cols), F32),
        w_proj,
        w_final,
        grant=None,
        name="mix",
    )
    frame_load, payload = smem_first(
        functools.partial(pack_body, extra, cols),
        (
            jax.ShapeDtypeStruct((frames, row_count + lat, model), BF16),
            jax.ShapeDtypeStruct((payload_rows, lanes), BF16),
        ),
        time_index,
        sched_index,
        w_qkv.transpose(1, 0, 2),
        start_noise,
        position,
        smem=2,
        scratch=(pltpu.VMEM((payload_rows + 1, lanes), F32), pltpu.VMEM((rows_d, lanes), F32)),
        grant=None,
        flops=4_000_000_000,
        name="pack",
    )

    mix = jnp.sum(lax.all_to_all(mix, "zlo", 0, 0, tiled=True), axis=0)
    mix = mix.reshape(lat // zlo_n, pieces, tall).transpose(2, 1, 0).reshape(tall, -1)
    payload = payload + jnp.pad(
        mix.astype(BF16), ((3 * rows_d, 1), (6 * extra, lanes - 6 * extra - mix.shape[1]))
    )

    frame_all = lax.all_to_all(frame_load, "frame", 0, 0, tiled=True)

    gathered = lax.all_gather(payload, STEP, axis=0)

    sides = gathered[:, 3 * rows_d : 3 * rows_d + tall]
    part = lat // zlo_n
    mixes = sides[:, :, 6 * extra :].astype(F32).reshape(zhi_n, zlo_n, tall, pieces, part)
    mixes = jnp.sum(mixes, axis=0).transpose(0, 3, 2, 1).reshape(lat, cols)
    mix_hi = lax.reduce_precision(mixes, 8, 7)
    wfp = jnp.concatenate([mix_hi, mixes - mix_hi], axis=0).astype(BF16)
    bext, a_all, c_all, base, fblk, coef, noise, states, x = smem_first(
        functools.partial(prep_body, lat, cores, extra),
        (
            jax.ShapeDtypeStruct((3 * cols + lat, tokens), F32),
            jax.ShapeDtypeStruct((3 * cols + lat, lanes), BF16),
            jax.ShapeDtypeStruct((steps, tokens), F32),
            jax.ShapeDtypeStruct((zlo_n, mine, lanes), F32),
            jax.ShapeDtypeStruct((3 * lanes, lanes), BF16),
            jax.ShapeDtypeStruct((2 * zlo_n, lanes), F32),
            jax.ShapeDtypeStruct((mine, lanes), F32),
            jax.ShapeDtypeStruct((zlo_n, mine, lanes), F32),
            jax.ShapeDtypeStruct((tokens, lanes), BF16),
        ),
        gathered,
        frame_all,
        position,
        start_noise,
        time_table,
        norm_gain.reshape(-1, lanes),
        coef_keep[None],
        coef_noise[None],
        w_in,
        w_final,
        scratch=(
            pltpu.VMEM((step_n, model), F32),
            pltpu.VMEM((row_count, lanes), F32),
            pltpu.VMEM((step_n * rows_d, 4 * lanes), F32),
            pltpu.VMEM((step_n, lanes), F32),
        ),
        name="prep",
    )

    squares = []
    for iteration in range(ITERS):
        part_eps = eps_part(x, bext, a_all, c_all, wfp, lat)
        got = lax.all_to_all(part_eps.reshape(members, mine, lanes), HOOD, 0, 0, tiled=True)
        if iteration < ITERS - 1:
            states, send, square = vmem_call(
                functools.partial(glue_body, lat, frames, cores),
                (
                    jax.ShapeDtypeStruct(states.shape, F32),
                    jax.ShapeDtypeStruct((members, mine, lanes), BF16),
                    jax.ShapeDtypeStruct((mine, lanes), F32),
                ),
                got,
                states,
                noise,
                base,
                fblk,
                coef,
                name="advance",
            )
            squares.append(square)
            x = lax.all_to_all(send, HOOD, 0, 0, tiled=True).reshape(tokens, lanes)
        else:
            send = smem_first(
                functools.partial(last_body, lat, frames, cores),
                jax.ShapeDtypeStruct((members, mine // 2, lanes), F32),
                        got,
                states,
                noise,
                base,
                fblk,
                coef,
                *squares,
                name="last",
            )
    ended = lax.all_to_all(send, HOOD, 0, 0, tiled=True)
    trajectory, norms = smem_first(
        functools.partial(end_body, lat, frames, cores, float(step_n * lat * tokens)),
        (
            jax.ShapeDtypeStruct((lat, row_count), F32),
            jax.ShapeDtypeStruct((ITERS,), F32),
        ),
        ended,
        scalars=(1,),
        name="end",
    )
    return trajectory[None], norms


def solution(mesh):
    names = ("parts", "zhi", "zlo", "frame", "head")
    sizes = mesh.shape
    devices = mesh.devices.reshape(
        sizes["parts"], sizes["step"] // ZLO, ZLO, sizes["frame"], sizes["head"]
    )
    return jax.shard_map(
        local,
        mesh=Mesh(devices, names),
        in_specs=(
            P("parts", "frame"),
            P("frame", None),
            P(),
            P(STEP),
            P(STEP),
            P(),
            P(),
            P(),
            P(),
            P(STEP, None, "head"),
            P(STEP, "head"),
            P(),
        ),
        out_specs=(P(STEP, "parts", "frame"), P("parts")),
        check_vma=False,
    )
```

```python
import functools
import math

import jax
import jax.numpy as jnp
from jax import lax
from jax.experimental import pallas as pl
from jax.experimental.pallas import tpu as pltpu
from jax.sharding import Mesh
from jax.sharding import PartitionSpec as P

HDIM = 72
ITERS = 4
ZLO = 4
GRANT = 16 * 1024 * 1024
F32 = jnp.float32
BF16 = jnp.bfloat16
STEP = ("zhi", "zlo")
HOOD = ("frame", "zlo", "head")


def chosen(pieces, index):
    out = pieces[0]
    for at, piece in enumerate(pieces[1:], 1):
        out = jnp.where(index == at, piece, out)
    return out


def vmem_call(body, out_shape, *args, scratch=(), flops=0, name=None):
    spec = pl.BlockSpec(memory_space=pltpu.VMEM)
    return pl.pallas_call(
        body,
        out_shape=out_shape,
        in_specs=[spec] * len(args),
        out_specs=jax.tree.map(lambda _: spec, out_shape),
        scratch_shapes=list(scratch),
        cost_estimate=pl.CostEstimate(flops=flops, bytes_accessed=0, transcendentals=0),
        compiler_params=pltpu.CompilerParams(vmem_limit_bytes=GRANT),
        name=name,
    )(*args)


def eps_body(heads, steps, lat, x_ref, bext_ref, a_ref, c_ref, wfp_ref, out_ref, xs, es, qs, ks, vs, os, s0, s1, m0, m1):
    cols = heads * HDIM
    tokens = x_ref.shape[0]
    xs[...] = x_ref[...].astype(F32).T
    scale = math.log2(math.e) / math.sqrt(HDIM)
    eight = lax.broadcasted_iota(jnp.int32, (steps, tokens), 0)
    blank = jnp.zeros((a_ref.shape[1] - 3 * (lat + steps), tokens), F32)
    ones8 = jnp.ones((8, tokens), F32)
    held, tops = (s0, s1), (m0, m1)

    lanes_pad = 128

    def project(step, carry):
        rows = pl.ds(pl.multiple_of(step * lat, lat), lat)
        x = xs[rows, :]
        pick = jnp.where(eight == step, 1.0, 0.0)
        xcat = jnp.concatenate([x, x, x, pick, pick, pick, blank], axis=0).astype(BF16)
        mixed = jnp.dot(a_ref[...], xcat, preferred_element_type=F32) + bext_ref[...]
        quad = mixed[3 * cols :, :]
        square = jnp.sum(x * quad, axis=0, keepdims=True) + c_ref[pl.ds(step, 1), :]
        rate = lax.rsqrt(jnp.maximum(square, 0.0) + 1e-06)
        for head in range(heads):
            q, k, v = (
                mixed[part * cols + head * HDIM : part * cols + (head + 1) * HDIM, :]
                for part in range(3)
            )
            qs[step, head] = (q * (rate * scale)).astype(BF16)
            ks[step, head] = (jnp.concatenate([k * rate, jnp.zeros((lanes_pad - HDIM, tokens), F32)], axis=0).T).astype(BF16)
            vs[step, head] = jnp.concatenate([v * rate, ones8], axis=0).astype(BF16)
        return carry

    lax.fori_loop(0, steps, project, 0, unroll=True)

    def score(step, head):
        s = jnp.dot(ks[step, head][:, :HDIM], qs[step, head], preferred_element_type=F32)
        held[head % 2][...] = s
        tops[head % 2][...] = jnp.max(s, axis=0, keepdims=True)

    def weigh(step, head):
        e = jnp.exp2(held[head % 2][...] - tops[head % 2][...]).astype(BF16)
        os[step, head] = jnp.dot(vs[step, head], e, preferred_element_type=F32)

    score(0, 0)

    def attend(step, carry):
        for head in range(heads):
            if head + 1 < heads:
                score(step, head + 1)
            else:
                score(jnp.minimum(step + 1, steps - 1), 0)
            weigh(step, head)
        return carry

    lax.fori_loop(0, steps, attend, 0, unroll=2)

    for step in range(steps):
        outs = []
        for head in range(heads):
            o = os[step, head]
            outs.append(o[:HDIM, :] * (1.0 / o[HDIM : HDIM + 1, :]))
        o = jnp.concatenate(outs, axis=0).astype(BF16)
        part = jnp.dot(wfp_ref[...], o, preferred_element_type=F32)
        es[step * lat : (step + 1) * lat, :] = part[:lat, :] + part[lat:, :]
    out_ref[...] = es[...].T.astype(BF16)


def eps_part(x, bext, a_all, c_all, wfp, lat):
    steps = c_all.shape[0]
    tokens = x.shape[0]
    heads = wfp.shape[1] // HDIM
    flops = 2 * steps * tokens * (bext.shape[0] * 64 + heads * tokens * 160)
    return vmem_call(
        functools.partial(eps_body, heads, steps, lat),
        jax.ShapeDtypeStruct((tokens, steps * lat), BF16),
        x,
        bext,
        a_all,
        c_all,
        wfp,
        scratch=(
            pltpu.VMEM((steps * lat, tokens), F32),
            pltpu.VMEM((steps * lat, tokens), F32),
            pltpu.VMEM((steps, heads, HDIM, tokens), BF16),
            pltpu.VMEM((steps, heads, tokens, 128), BF16),
            pltpu.VMEM((steps, heads, HDIM + 8, tokens), BF16),
            pltpu.VMEM((steps, heads, HDIM + 8, tokens), F32),
            pltpu.VMEM((tokens, tokens), F32),
            pltpu.VMEM((tokens, tokens), F32),
            pltpu.VMEM((1, tokens), F32),
            pltpu.VMEM((1, tokens), F32),
        ),
        flops=flops,
        name="eps_part",
    )


def advance(lat, frames, cores, got_ref, x_ref, noise_ref, base_ref, fblk_ref, coef_ref):
    groups, rows, lanes = x_ref.shape
    lane = lax.broadcasted_iota(jnp.int32, (rows, lanes), 1)
    before = jnp.zeros((rows, lanes), F32)
    drifts, states = [], []
    square = jnp.zeros((rows, lanes), F32)
    for group in range(groups):
        old = x_ref[group]
        total = base_ref[group]
        for frame in range(frames):
            for core in range(cores):
                member = (frame * groups + group) * cores + core
                total = total + got_ref[member].astype(F32)
        xb = old.astype(BF16)
        total = total + jnp.dot(
            jnp.concatenate([xb, xb, xb], axis=1), fblk_ref[...], preferred_element_type=F32
        )
        drift = (
            coef_ref[pl.ds(group, 1), :] * old + coef_ref[pl.ds(groups + group, 1), :] * total
        )
        running = drift
        shift = lat
        while shift < lanes:
            running = running + jnp.where(lane >= shift, pltpu.roll(running, shift, 1), 0.0)
            shift *= 2
        own = jnp.where(lane >= lat, pltpu.roll(running, lat, 1), 0.0)
        new = noise_ref[...] + before + own
        last = jnp.where(lane >= lanes - lat, running, 0.0)
        shift = lanes // 2
        while shift >= lat:
            last = last + pltpu.roll(last, shift, 1)
            shift //= 2
        before = before + last
        change = new - old
        square = square + change * change
        drifts.append(drift)
        states.append(new)
    return drifts, states, square


def glue_body(lat, frames, cores, got_ref, x_ref, noise_ref, base_ref, fblk_ref, coef_ref,
              new_ref, send_ref, square_ref):
    _, states, square = advance(
        lat, frames, cores, got_ref, x_ref, noise_ref, base_ref, fblk_ref, coef_ref
    )
    square_ref[...] = square
    groups = len(states)
    for group, new in enumerate(states):
        new_ref[group] = new
        rounded = new.astype(BF16)
        for frame in range(frames):
            for core in range(cores):
                send_ref[(frame * groups + group) * cores + core] = rounded


def last_body(lat, frames, cores, got_ref, x_ref, noise_ref, base_ref, fblk_ref,
              coef_ref, sq0_ref, sq1_ref, sq2_ref, send_ref):
    drifts, states, square = advance(
        lat, frames, cores, got_ref, x_ref, noise_ref, base_ref, fblk_ref, coef_ref
    )
    groups, rows, lanes = x_ref.shape
    half = rows // 2
    zhi = lax.axis_index("zhi")
    width = groups * lat
    first = zhi * groups
    per_group = lanes // lat
    picked = chosen([s + d for s, d in zip(states, drifts)], first // per_group)
    offset = lax.rem(first, per_group) * lat
    lane = lax.broadcasted_iota(jnp.int32, (half, lanes), 1)
    turn = lax.rem(lanes - offset, lanes)
    top = pltpu.roll(picked[:half], turn, 1)
    bottom = pltpu.roll(picked[half:], lax.rem(turn + width, lanes), 1)
    piece = jnp.where(lane < width, top, bottom)
    sums = jnp.zeros((half, lanes), F32)
    inner = lax.rem(lane, lat)
    for at, sq in enumerate((sq0_ref[...], sq1_ref[...], sq2_ref[...], square)):
        sums = jnp.where(inner == at, jnp.sum(sq), sums)
    for group in range(groups):
        slot = (group + 1) % groups
        mixed = jnp.where(lane // lat == slot, sums, piece)
        for frame in range(frames):
            for core in range(cores):
                send_ref[(frame * groups + group) * cores + core] = mixed


def end_body(lat, frames, cores, cells, got_ref, traj_ref, norm_ref):
    members, half, lanes = got_ref.shape
    groups = members // (frames * cores)
    frame, zlo = lax.axis_index("frame"), lax.axis_index("zlo")
    width = groups * lat
    everyone = got_ref[0]
    for member in range(1, members):
        everyone = everyone + got_ref[member]
    slot = lax.rem(zlo + 1, groups)
    sums = pltpu.roll(everyone, lax.rem(lanes - slot * lat, lanes), 1)
    norms = jnp.sqrt(sums[:1] / cells + 1e-06)
    for at in range(ITERS):
        norm_ref[at] = norms[0, at]
    rows = []
    back = lax.rem(lanes - zlo * lat, lanes)
    for own in range(groups * cores):
        piece = got_ref[frame * (groups * cores) + own]
        rows.append(pltpu.roll(piece, back, 1))
        rows.append(pltpu.roll(piece, lax.rem(back + lanes - width, lanes), 1))
    traj_ref[...] = jnp.concatenate(rows, axis=0).T[:lat, :]


def smem_first(body, out_shape, *args, smem=0, scratch=(), grant=GRANT, scalars=(), flops=0, name=None):
    spec = pl.BlockSpec(memory_space=pltpu.VMEM)
    held = pl.BlockSpec(memory_space=pltpu.SMEM)
    out_specs = jax.tree.map(lambda _: spec, out_shape)
    for at in scalars:
        out_specs = (*out_specs[:at], held, *out_specs[at + 1 :])
    return pl.pallas_call(
        body,
        out_shape=out_shape,
        in_specs=[held] * smem + [spec] * (len(args) - smem),
        out_specs=out_specs,
        scratch_shapes=list(scratch),
        cost_estimate=pl.CostEstimate(flops=flops, bytes_accessed=0, transcendentals=0),
        compiler_params=pltpu.CompilerParams(vmem_limit_bytes=grant),
        name=name,
    )(*args)


def split_two(a):
    hi = a.astype(BF16)
    return hi, (a - hi.astype(F32)).astype(BF16)


def split_lanes(a, lat, steps):
    hi = a.astype(BF16).astype(F32)
    mid = (a - hi).astype(BF16).astype(F32)
    low = a - hi - mid
    lane = lax.broadcasted_iota(jnp.int32, a.shape, 1)
    first, second, third = 3 * lat, 3 * lat + steps, 3 * lat + 2 * steps
    is_hi = (lane < lat) | ((lane >= first) & (lane < second))
    is_mid = ((lane >= lat) & (lane < 2 * lat)) | ((lane >= second) & (lane < third))
    return jnp.where(is_hi, hi, jnp.where(is_mid, mid, low)).astype(BF16)


def prep_body(lat, cores, extra, got_ref, all_ref, position_ref, start_ref, table_ref,
              gain_ref, keep_ref, rate_ref, w_in_ref, final_ref, bext_ref, a_ref, c_ref, base_ref, fblk_ref, coef_ref, noise_ref, state_ref, x_ref,
              temb_ref, turned_ref, w_ref, index_ref):
    zlo, core = lax.axis_index("zlo"), lax.axis_index("head")
    frames = all_ref.shape[0]
    rows, model = position_ref.shape
    groups, mine, lanes = base_ref.shape
    steps = lanes // lat
    count = groups * steps
    inv = 1.0 / model
    nt = (((1,), (1,)), ((), ()))

    def nt_dot(a, b):
        return lax.dot_general(a, b, nt, preferred_element_type=F32)

    rows_d = model // count
    tall = rows_d // 2
    for source in range(count):
        got = got_ref[source].astype(F32)
        at = source * rows_d
        for part in range(3):
            w_ref[at : at + rows_d, part * lanes : (part + 1) * lanes] = got[
                part * rows_d : (part + 1) * rows_d
            ]
        side = got[3 * rows_d : 3 * rows_d + tall]
        w_ref[at : at + tall, 3 * lanes :] = side
        w_ref[at + tall : at + rows_d, 3 * lanes :] = jnp.concatenate(
            [side[:, 3 * extra :], side[:, : 3 * extra]], axis=1
        )
        index_ref[source : source + 1] = got[3 * rows_d + tall : 3 * rows_d + tall + 1]

    spots = lax.broadcasted_iota(jnp.int32, (count, table_ref.shape[0]), 1).astype(F32)
    pick_time = jnp.where(index_ref[:, 0:1] == spots, 1.0, 0.0).astype(BF16)
    pick_sched = jnp.where(index_ref[:, 1:2] == spots, 1.0, 0.0)
    temb_all = jnp.dot(pick_time, table_ref[...], preferred_element_type=F32)
    temb_ref[...] = temb_all
    temb = temb_ref[pl.ds(pl.multiple_of(zlo * steps, steps), steps), :]
    lane = lax.broadcasted_iota(jnp.int32, (count, lanes), 1)
    own = lax.broadcasted_iota(jnp.int32, (count, lanes), 0)
    here = (lane // lat) == lax.rem(own, steps)

    def spread(a):
        return jnp.sum(jnp.where(here, a, 0.0).reshape(groups, steps, lanes), axis=1)

    keep = jnp.sum(pick_sched * keep_ref[...], axis=1, keepdims=True)
    rate = jnp.sum(pick_sched * rate_ref[...], axis=1, keepdims=True)
    coef_ref[:groups] = spread(jnp.broadcast_to(keep, (count, lanes)))
    coef_ref[groups:] = spread(jnp.broadcast_to(rate, (count, lanes)))

    final = final_ref[...].astype(F32)
    final = jnp.concatenate([final] * steps, axis=0).astype(BF16)
    w_in = w_in_ref[...].astype(F32)
    w_in_all = jnp.concatenate([w_in] * steps, axis=0).astype(BF16)
    mixed = nt_dot(w_in_all, final)
    square_lane = lax.broadcasted_iota(jnp.int32, (lanes, lanes), 1) // lat
    square_row = lax.broadcasted_iota(jnp.int32, (lanes, lanes), 0) // lat
    mixed = jnp.where(square_lane == square_row, mixed, 0.0)
    hi = mixed.astype(BF16)
    mid = (mixed - hi.astype(F32)).astype(BF16)
    fblk_ref[:lanes] = hi
    fblk_ref[lanes : 2 * lanes] = mid
    fblk_ref[2 * lanes :] = (mixed - hi.astype(F32) - mid.astype(F32)).astype(BF16)
    at = pl.multiple_of((zlo * cores + core) * mine, mine)
    base_own = nt_dot(position_ref[pl.ds(at, mine), :], final)
    base_time = spread(nt_dot(temb_all.astype(BF16), final))
    for group in range(groups):
        base_ref[group] = base_own + base_time[group : group + 1, :]

    turned_ref[...] = jnp.concatenate([start_ref[...]] * steps, axis=0).T
    noise = turned_ref[pl.ds(at, mine), :]
    noise_ref[...] = noise
    for group in range(groups):
        state_ref[group] = noise
    for frame in range(frames):
        noise = all_ref[frame, rows:, :rows].astype(F32)
        x_ref[frame * rows : (frame + 1) * rows] = (
            jnp.concatenate([noise] * steps, axis=0).T.astype(BF16)
        )

    blank = jnp.zeros((lanes - 3 * (lat + steps), model), F32)
    thin = jnp.concatenate([w_in, w_in, w_in, temb, temb, temb, blank], axis=0)
    thin_bf = thin.astype(BF16)
    gain = jnp.concatenate([gain_ref[at : at + 1] for at in range(model // lanes)], axis=1)
    w = w_ref[...].astype(BF16)
    thin_hi, thin_lo = split_two(thin * gain)
    linear = jnp.dot(thin_hi, w, preferred_element_type=F32) + jnp.dot(
        thin_lo, w, preferred_element_type=F32
    )
    places = []
    for part in range(3):
        places += [(part * lanes, lanes), (3 * lanes + part * extra, extra)]
    row = 0
    turned = linear.T
    for start, size in places:
        a_ref[row : row + size] = split_lanes(turned[start : start + size], lat, steps)
        row += size
    gram = nt_dot(thin_bf[:lat], thin_bf)
    gram_lane = lax.broadcasted_iota(jnp.int32, gram.shape, 1)
    gram = gram * jnp.where(gram_lane < 3 * lat, inv, 2.0 * inv)
    a_ref[row:] = split_lanes(gram, lat, steps)
    temb_square = jnp.sum(temb * temb, axis=1, keepdims=True)
    for frame in range(frames):
        there = pl.ds(frame * rows, rows)
        tokens_bf = all_ref[frame, :rows, :]
        wide = tokens_bf.astype(F32)
        wide_hi, wide_lo = split_two(wide * gain)
        linear = (
            jnp.dot(wide_hi, w, preferred_element_type=F32)
            + jnp.dot(wide_lo, w, preferred_element_type=F32)
        ).T
        row = 0
        for start, size in places:
            bext_ref[row : row + size, frame * rows : (frame + 1) * rows] = linear[
                start : start + size
            ]
            row += size
        gram = nt_dot(thin_bf, tokens_bf)
        bext_ref[row:, frame * rows : (frame + 1) * rows] = gram[:lat] * (2.0 * inv)
        square = wide * wide
        folded = square[:, :lanes]
        for chunk in range(1, model // lanes):
            folded = folded + square[:, chunk * lanes : (chunk + 1) * lanes]
        square = jnp.sum(folded.T, axis=0, keepdims=True)
        c_ref[:, frame * rows : (frame + 1) * rows] = inv * (
            square + 2.0 * gram[3 * lat : 3 * lat + steps] + temb_square
        )


def exact_pick(values, wanted):
    return jnp.dot(values, jnp.where(wanted, 1.0, 0.0).astype(BF16), preferred_element_type=F32)


def mix_body(proj_ref, final_ref, mix_ref):
    frame = lax.axis_index("frame")
    step = lax.axis_index("zhi") * lax.axis_size("zlo") + lax.axis_index("zlo")
    lat, model = final_ref.shape
    rows_d, width = proj_ref.shape
    parts, each, cols = mix_ref.shape
    lanes = 128
    column = lax.broadcasted_iota(jnp.int32, (width, 2 * lanes), 0) - frame * cols
    both = column == lax.broadcasted_iota(jnp.int32, (width, 2 * lanes), 1)
    feature = lax.broadcasted_iota(jnp.int32, (model, lanes), 0) - step * rows_d
    final = exact_pick(final_ref[...], feature == lax.broadcasted_iota(jnp.int32, (model, lanes), 1))
    proj = exact_pick(proj_ref[...], both)
    blank = jnp.zeros((lanes - rows_d, 2 * lanes), F32)
    proj = jnp.concatenate([proj, blank], axis=0).astype(BF16)
    feature_lane = lax.broadcasted_iota(jnp.int32, final.shape, 1)
    final = jnp.where(feature_lane < rows_d, final, 0.0).astype(BF16)
    mix = jnp.dot(final, proj, preferred_element_type=F32)
    for part in range(parts):
        mix_ref[part] = mix[part * each : (part + 1) * each, :cols]


def pack_body(extra, cols, time_ref, plan_ref, qkv_ref, start_ref, position_ref,
              frame_ref, main_ref, rows_ref, half_ref):
    frame = lax.axis_index("frame")
    lat, rows = start_ref.shape
    rows_d, width = qkv_ref.shape[1:]
    frames = frame_ref.shape[0]
    lanes = main_ref.shape[1]
    tall = rows_d // 2

    column = lax.broadcasted_iota(jnp.int32, (width, 2 * lanes), 0) - frame * cols
    lane = lax.broadcasted_iota(jnp.int32, (width, 2 * lanes), 1)
    both = column == lane
    model = position_ref.shape[1]

    noise = jnp.concatenate(
        [start_ref[...], jnp.zeros((lat, model - rows), F32)], axis=1
    ).astype(BF16)
    for at in range(frames):
        frame_ref[at, :rows] = position_ref[...]
        frame_ref[at, rows:] = noise

    side = jnp.zeros(half_ref.shape, F32)
    place = lax.broadcasted_iota(jnp.int32, half_ref.shape, 1)
    for part in range(3):
        picked = exact_pick(qkv_ref[part], both)
        rows_ref[part * rows_d : (part + 1) * rows_d, :] = picked[:, :lanes]
        half_ref[:rows_d, :] = picked[:, lanes:]
        rest = jnp.where(place < extra, half_ref[...], 0.0)
        side = side + (pltpu.roll(rest, part * extra, 1) if part else rest)
    half_ref[...] = pltpu.roll(side, 3 * extra, 1)
    rows_ref[3 * rows_d : 3 * rows_d + tall, :] = side[:tall] + half_ref[tall:rows_d, :]
    spot = lax.broadcasted_iota(jnp.int32, (1, lanes), 1)
    times = time_ref[0].astype(F32)
    plans = plan_ref[0].astype(F32)
    rows_ref[3 * rows_d + tall : 3 * rows_d + tall + 1, :] = jnp.where(
        spot == 0, times, jnp.where(spot == 1, plans, 0.0)
    )
    main_ref[...] = rows_ref[...][: main_ref.shape[0], :].astype(BF16)


def local(
    start_noise,
    position,
    time_table,
    time_index,
    sched_index,
    coef_keep,
    coef_noise,
    w_in,
    norm_gain,
    w_qkv,
    w_proj,
    w_final,
):
    lat, row_count = start_noise.shape
    rows_d = w_qkv.shape[0]
    model = position.shape[1]
    frames, cores = lax.axis_size("frame"), lax.axis_size("head")
    zlo_n, zhi_n = lax.axis_size("zlo"), lax.axis_size("zhi")
    step_n = zlo_n * zhi_n
    steps = step_n // zlo_n
    tokens = row_count * frames
    cols = w_qkv.shape[2] // frames
    heads = cols // HDIM
    members = frames * zlo_n * cores
    mine = tokens // members
    lanes = steps * lat

    tall = rows_d // 2
    extra = cols - lanes
    pieces = cols // tall
    payload_rows = 3 * rows_d + tall + 1
    mix = smem_first(
        mix_body,
        jax.ShapeDtypeStruct((zlo_n, lat // zlo_n, cols), F32),
        w_proj,
        w_final,
        grant=None,
        name="mix",
    )
    frame_load, payload = smem_first(
        functools.partial(pack_body, extra, cols),
        (
            jax.ShapeDtypeStruct((frames, row_count + lat, model), BF16),
            jax.ShapeDtypeStruct((payload_rows, lanes), BF16),
        ),
        time_index,
        sched_index,
        w_qkv.transpose(1, 0, 2),
        start_noise,
        position,
        smem=2,
        scratch=(pltpu.VMEM((payload_rows + 1, lanes), F32), pltpu.VMEM((rows_d + 4, lanes), F32)),
        grant=None,
        flops=4_000_000_000,
        name="pack",
    )

    mix = jnp.sum(lax.all_to_all(mix, "zlo", 0, 0, tiled=True), axis=0)
    mix = mix.reshape(lat // zlo_n, pieces, tall).transpose(2, 1, 0).reshape(tall, -1)
    payload = payload + jnp.pad(
        mix.astype(BF16), ((3 * rows_d, 1), (6 * extra, lanes - 6 * extra - mix.shape[1]))
    )

    frame_all = lax.all_to_all(frame_load, "frame", 0, 0, tiled=True)

    gathered = lax.all_gather(payload, STEP, axis=0)

    sides = gathered[:, 3 * rows_d : 3 * rows_d + tall]
    part = lat // zlo_n
    mixes = sides[:, :, 6 * extra :].astype(F32).reshape(zhi_n, zlo_n, tall, pieces, part)
    mixes = jnp.sum(mixes, axis=0).transpose(0, 3, 2, 1).reshape(lat, cols)
    mix_hi = lax.reduce_precision(mixes, 8, 7)
    wfp = jnp.concatenate([mix_hi, mixes - mix_hi], axis=0).astype(BF16)
    bext, a_all, c_all, base, fblk, coef, noise, states, x = smem_first(
        functools.partial(prep_body, lat, cores, extra),
        (
            jax.ShapeDtypeStruct((3 * cols + lat, tokens), F32),
            jax.ShapeDtypeStruct((3 * cols + lat, lanes), BF16),
            jax.ShapeDtypeStruct((steps, tokens), F32),
            jax.ShapeDtypeStruct((zlo_n, mine, lanes), F32),
            jax.ShapeDtypeStruct((3 * lanes, lanes), BF16),
            jax.ShapeDtypeStruct((2 * zlo_n, lanes), F32),
            jax.ShapeDtypeStruct((mine, lanes), F32),
            jax.ShapeDtypeStruct((zlo_n, mine, lanes), F32),
            jax.ShapeDtypeStruct((tokens, lanes), BF16),
        ),
        gathered,
        frame_all,
        position,
        start_noise,
        time_table,
        norm_gain.reshape(-1, lanes),
        coef_keep[None],
        coef_noise[None],
        w_in,
        w_final,
        scratch=(
            pltpu.VMEM((step_n, model), F32),
            pltpu.VMEM((row_count, lanes), F32),
            pltpu.VMEM((step_n * rows_d, 4 * lanes), F32),
            pltpu.VMEM((step_n, lanes), F32),
        ),
        name="prep",
    )

    squares = []
    for iteration in range(ITERS):
        part_eps = eps_part(x, bext, a_all, c_all, wfp, lat)
        got = lax.all_to_all(part_eps.reshape(members, mine, lanes), HOOD, 0, 0, tiled=True)
        if iteration < ITERS - 1:
            states, send, square = vmem_call(
                functools.partial(glue_body, lat, frames, cores),
                (
                    jax.ShapeDtypeStruct(states.shape, F32),
                    jax.ShapeDtypeStruct((members, mine, lanes), BF16),
                    jax.ShapeDtypeStruct((mine, lanes), F32),
                ),
                got,
                states,
                noise,
                base,
                fblk,
                coef,
                name="advance",
            )
            squares.append(square)
            x = lax.all_to_all(send, HOOD, 0, 0, tiled=True).reshape(tokens, lanes)
        else:
            send = smem_first(
                functools.partial(last_body, lat, frames, cores),
                jax.ShapeDtypeStruct((members, mine // 2, lanes), F32),
                        got,
                states,
                noise,
                base,
                fblk,
                coef,
                *squares,
                name="last",
            )
    ended = lax.all_to_all(send, HOOD, 0, 0, tiled=True)
    trajectory, norms = smem_first(
        functools.partial(end_body, lat, frames, cores, float(step_n * lat * tokens)),
        (
            jax.ShapeDtypeStruct((lat, row_count), F32),
            jax.ShapeDtypeStruct((ITERS,), F32),
        ),
        ended,
        scalars=(1,),
        name="end",
    )
    return trajectory[None], norms


def solution(mesh):
    names = ("parts", "zhi", "zlo", "frame", "head")
    sizes = mesh.shape
    devices = mesh.devices.reshape(
        sizes["parts"], sizes["step"] // ZLO, ZLO, sizes["frame"], sizes["head"]
    )
    return jax.shard_map(
        local,
        mesh=Mesh(devices, names),
        in_specs=(
            P("parts", "frame"),
            P("frame", None),
            P(),
            P(STEP),
            P(STEP),
            P(),
            P(),
            P(),
            P(),
            P(STEP, None, "head"),
            P(STEP, "head"),
            P(),
        ),
        out_specs=(P(STEP, "parts", "frame"), P("parts")),
        check_vma=False,
    )
```
